32 devices in a mesh: graph: 8 (over y, x, core), rep: 4 (over z).
Axes of the slice: x: 2, y: 2, z: 4, core: 2. Of those that a mesh axis runs over, the one named last changes fastest.
Arguments:
- nodes: bfloat16 [4, 64, 32, 256], P('rep', 'graph'), may hold values from -20 to 20, as said below
- cotangent: bfloat16 [4, 64, 32, 256], P('rep', 'graph'), may hold values from -6 to 6
- live: int32 [4, 64], P('rep', 'graph'), may hold values from 2 to 32, as said below
- partner_first: int32 [4, 64], P('rep', 'graph'), may hold values from 0 to 63, as said below
- partner_size: int32 [4, 64], P('rep', 'graph'), may hold values from 1 to 2
- edge_src: int32 [4, 2048], P('rep', 'graph'), may hold values from 0 to 255, as said below
- edge_dst: int32 [4, 2048], P('rep', 'graph'), may hold values from 0 to 255, as said below
- w_edge1: bfloat16 [512, 512], replicated, may hold values from -0.25 to 0.25
- b_edge: float32 [512], replicated, may hold values from -3 to 3
- w_edge2: bfloat16 [512, 256], replicated, may hold values from -0.25 to 0.25
- w_node1: bfloat16 [768, 512], replicated, may hold values from -0.21875 to 0.21875
- b_node: float32 [512], replicated, may hold values from -3 to 3
- w_node2: bfloat16 [512, 256], replicated, may hold values from -0.25 to 0.25
Outputs:
- updated: bfloat16 [4, 64, 32, 256], P('rep', 'graph')
- d_nodes: bfloat16 [4, 64, 32, 256], P('rep', 'graph')
- g_edge1: float32 [512, 512], P('rep')
- g_bedge: float32 [512], P('rep')
- g_edge2: float32 [512, 256], P('rep')
- g_node1: float32 [768, 512], P('rep')
- g_bnode: float32 [512], P('rep')
- g_node2: float32 [512, 256], P('rep')
The draws below stay inside these ranges and needn't reach their ends.
Inputs may be any that keep to these rules, and one draw needn't show every extreme that they name: A graph is one or two consecutive granules of one device, and every granule of a graph but its last is full; rows beyond live are padding. `partner_first`: index within the replica of the first granule of the partner graph, the same for all granules of a graph; pairing is mutual. Graphs in the lower half of a device's 8 granules pair with graphs in the upper half of some device's granules; the upper-half graphs of one device have partners on distinct devices. Within a replica every half of every device holds the same number of two-granule graphs. `edge_src`: row index within the device (granule times 32 plus row); both ends of an edge are live rows of the same graph. `edge_dst`: as edge_src. `nodes`: padding rows are zero.
All inputs are finite; a program needn't handle non-finite values.
Results may differ from the reference program's by a relative error of at most 0.023.
Values may be sent and summed in bfloat16 or wider, within the bound.
A program may use at most 128 MiB of HBM per device.

```python
import jax
import jax.numpy as jnp
from jax import lax

H = 256
FM = 512
BLK = 32
GMAX = 2
NB = 8
E_DEV = 256
G_ALL = 64
N_GRAPH = 8
N_REP = 4


def inverse_order(ordering):
    return jnp.zeros(ordering.shape, jnp.int32).at[ordering].set(jnp.arange(ordering.shape[0], dtype=jnp.int32))


def device_orders(stream):
    streams = jax.random.split(stream, N_GRAPH)
    return jax.vmap(lambda single: inverse_order(jax.random.permutation(single, N_GRAPH).astype(jnp.int32)))(streams)


def pick(member, lookup):
    return jnp.sum(jnp.where(member, lookup, 0), axis=2).astype(jnp.int32)


def layout_one(replica_key):
    peer_count = N_GRAPH
    half_count = NB // 2
    streams = jax.random.split(jax.random.fold_in(replica_key, 17), 8)
    lowest = max(half_count - peer_count, 1)
    highest = half_count // 2
    double_count = jax.random.randint(streams[0], (), lowest, highest + 1)
    graph_count = half_count - double_count
    offsets = jnp.arange(peer_count, dtype=jnp.int32)
    first_order = inverse_order(jax.random.permutation(streams[1], peer_count).astype(jnp.int32))
    active = first_order < graph_count
    size_moving = jnp.where(active, jnp.where(first_order < double_count, 2, 1), 0).astype(jnp.int32)
    second_order = inverse_order(jax.random.permutation(streams[2], peer_count).astype(jnp.int32))
    rank_active = jnp.sum(active[None, :] & (second_order[None, :] < second_order[:, None]), axis=1)
    size_staying = jnp.where(active, jnp.where(rank_active < double_count, 2, 1), 0).astype(jnp.int32)
    sigma = jax.random.permutation(streams[3], peer_count).astype(jnp.int32)
    sigma_inverse = inverse_order(sigma)
    tau = jax.random.permutation(streams[4], peer_count).astype(jnp.int32)
    tau_inverse = inverse_order(tau)
    order_moving = device_orders(streams[5])
    order_staying = device_orders(streams[6])
    start_moving = jnp.sum(size_moving[None, None, :] * (order_moving[:, None, :] < order_moving[:, :, None]), axis=2).astype(jnp.int32)
    start_staying = jnp.sum(size_staying[None, None, :] * (order_staying[:, None, :] < order_staying[:, :, None]), axis=2).astype(jnp.int32)
    staying_device = sigma_inverse[(tau[:, None] + offsets[None, :]) % peer_count]
    moving_device = tau_inverse[(sigma[:, None] - offsets[None, :]) % peer_count]
    spots = jnp.arange(half_count, dtype=jnp.int32)
    member_staying = active[None, None, :] & (start_staying[:, None, :] <= spots[None, :, None]) & (spots[None, :, None] < start_staying[:, None, :] + size_staying[None, None, :])
    member_moving = active[None, None, :] & (start_moving[:, None, :] <= spots[None, :, None]) & (spots[None, :, None] < start_moving[:, None, :] + size_moving[None, None, :])
    offset_low = pick(member_staying, offsets[None, None, :])
    first_low = pick(member_staying, start_staying[:, None, :])
    size_low = pick(member_staying, size_staying[None, None, :])
    mate_low = jnp.take_along_axis(moving_device, offset_low, axis=1)
    partner_low = mate_low * NB + half_count + start_moving[mate_low, offset_low]
    mate_size_low = size_moving[offset_low]
    offset_high = pick(member_moving, offsets[None, None, :])
    first_high = pick(member_moving, start_moving[:, None, :]) + half_count
    size_high = pick(member_moving, size_moving[None, None, :])
    mate_high = jnp.take_along_axis(staying_device, offset_high, axis=1)
    partner_high = mate_high * NB + start_staying[mate_high, offset_high]
    mate_size_high = size_staying[offset_high]
    partner = jnp.concatenate([partner_low, partner_high], axis=1).astype(jnp.int32)
    partner_sizes = jnp.concatenate([mate_size_low, mate_size_high], axis=1).astype(jnp.int32)
    own_local = jnp.concatenate([first_low, first_high], axis=1)
    own_size = jnp.concatenate([size_low, size_high], axis=1)
    place_index = jnp.arange(NB, dtype=jnp.int32)[None, :] - own_local
    lowest_live = max(2, BLK // 4)
    live_counts = jax.random.randint(streams[7], (peer_count, NB), lowest_live, BLK + 1)
    live_counts = jnp.where((own_size == 2) & (place_index == 0), BLK, live_counts).astype(jnp.int32)
    own_first = (jnp.arange(peer_count, dtype=jnp.int32)[:, None] * NB + own_local).astype(jnp.int32)
    return (live_counts.reshape(-1), partner.reshape(-1), partner_sizes.reshape(-1), own_first.reshape(-1), own_size.reshape(-1).astype(jnp.int32))


def edges_one(replica_key):
    live_counts, partner, partner_sizes, own_first, own_size = layout_one(replica_key)
    streams = jax.random.split(jax.random.fold_in(replica_key, 29), 4)
    device_base = jnp.arange(N_GRAPH, dtype=jnp.int32)[:, None] * NB
    target_local = jax.random.randint(streams[0], (N_GRAPH, E_DEV), 0, NB)
    target_granule = device_base + target_local
    target_row = jax.random.randint(streams[1], (N_GRAPH, E_DEV), 0, live_counts[target_granule])
    source_granule = own_first[target_granule] + jax.random.randint(streams[2], (N_GRAPH, E_DEV), 0, own_size[target_granule])
    source_row = jax.random.randint(streams[3], (N_GRAPH, E_DEV), 0, live_counts[source_granule])
    source_local = (source_granule - device_base) * BLK + source_row
    target_flat = target_local * BLK + target_row
    return (source_local.reshape(-1).astype(jnp.int32), target_flat.reshape(-1).astype(jnp.int32))


def nodes_one(replica_key):
    live_counts, partner, partner_sizes, own_first, own_size = layout_one(replica_key)
    streams = jax.random.split(jax.random.fold_in(replica_key, 41), 1)
    granules = N_GRAPH * NB
    values = jnp.clip(jax.random.normal(streams[0], (granules, BLK, H), jnp.float32), -6.0, 6.0)
    row_live = jnp.arange(BLK, dtype=jnp.int32)[None, :] < live_counts[:, None]
    return jnp.where(row_live[:, :, None], values, 0.0)


def over_replicas(key, maker):
    return jax.vmap(lambda replica_index: maker(jax.random.fold_in(key, replica_index)))(jnp.arange(N_REP, dtype=jnp.int32))


def draw_nodes(key, part):
    return over_replicas(key, nodes_one).astype(jnp.bfloat16)


def draw_live(key, part):
    return over_replicas(key, lambda replica_key: layout_one(replica_key)[0])


def draw_partner_first(key, part):
    return over_replicas(key, lambda replica_key: layout_one(replica_key)[1])


def draw_partner_size(key, part):
    return over_replicas(key, lambda replica_key: layout_one(replica_key)[2])


def draw_edge_src(key, part):
    return over_replicas(key, lambda replica_key: edges_one(replica_key)[0])


def draw_edge_dst(key, part):
    return over_replicas(key, lambda replica_key: edges_one(replica_key)[1])


def level_of(rng, extent, cuts, smallest, high):
    def one(dim, blocks):
        draws = jax.random.uniform(jax.random.fold_in(jax.random.fold_in(rng, 6), dim), (blocks,), jnp.float32, smallest / len(cuts), high / len(cuts))
        return jnp.repeat(jnp.exp(draws), extent[dim] // blocks).reshape((-1,) + (1,) * (len(extent) - dim - 1))

    level = one(*cuts[0])
    for cut in cuts[1:]:
        level = level * one(*cut)
    return level


def centred(key, extent, deviation, bound, cuts=(), kind=jnp.bfloat16):
    result = jax.random.normal(key, extent, jnp.float32) * deviation
    if len(cuts) > 0:
        result = level_of(key, extent, cuts, -0.22, 0.18) * result
    return jnp.clip(result, min=-bound, max=bound).astype(kind)


def setup_inputs(seed: int = 0) -> dict:
    key_of = jax.random.split(jax.random.key(seed), 14)
    return {
        "nodes": draw_nodes(jax.random.fold_in(key_of[13], 71), 0),
        "cotangent": centred(key_of[1], (N_REP, G_ALL, BLK, H), 1.0, 6.0, ((0, 4), (1, 8))),
        "live": draw_live(jax.random.fold_in(key_of[13], 71), 0),
        "partner_first": draw_partner_first(jax.random.fold_in(key_of[13], 71), 0),
        "partner_size": draw_partner_size(jax.random.fold_in(key_of[13], 71), 0),
        "edge_src": draw_edge_src(jax.random.fold_in(key_of[13], 71), 0),
        "edge_dst": draw_edge_dst(jax.random.fold_in(key_of[13], 71), 0),
        "w_edge1": centred(key_of[7], (2 * H, FM), (2 * H) ** -0.5, 0.25),
        "b_edge": centred(key_of[8], (FM,), 0.5, 3.0, (), jnp.float32),
        "w_edge2": centred(key_of[9], (FM, H), FM ** -0.5, 0.25),
        "w_node1": centred(key_of[10], (3 * H, FM), (3 * H) ** -0.5, 0.21875),
        "b_node": centred(key_of[11], (FM,), 0.5, 3.0, (), jnp.float32),
        "w_node2": centred(key_of[12], (FM, H), FM ** -0.5, 0.25),
    }


def silu_slope(values):
    sigmoid_value = jax.nn.sigmoid(values)
    return sigmoid_value * (1.0 + values * (1.0 - sigmoid_value))


def attend(queries, key_rows, key_mask):
    scale_factor = queries.shape[-1] ** -0.5
    scores = jnp.einsum("gqh,gkh->gqk", queries.astype(jnp.float32), key_rows.astype(jnp.float32), precision=lax.Precision.HIGHEST) * scale_factor
    scores = jnp.where(key_mask[:, None, :], scores, -jnp.inf)
    highest = jnp.max(scores, axis=-1, keepdims=True)
    powers = jnp.exp(scores - highest)
    softmax_out = powers / jnp.sum(powers, axis=-1, keepdims=True)
    softmax_low = softmax_out.astype(jnp.bfloat16)
    context = jnp.einsum("gqk,gkh->gqh", softmax_low.astype(jnp.float32), key_rows.astype(jnp.float32), precision=lax.Precision.HIGHEST)
    moved_rows = (queries.astype(jnp.float32) - context).astype(jnp.bfloat16)
    return moved_rows, softmax_out, softmax_low


def attend_back(queries, key_rows, softmax_out, softmax_low, grad_moved):
    scale_factor = queries.shape[-1] ** -0.5
    negated = (-grad_moved).astype(jnp.float32)
    keys_wide = key_rows.astype(jnp.float32)
    grad_probs = jnp.einsum("gqh,gkh->gqk", negated, keys_wide, precision=lax.Precision.HIGHEST)
    grad_keys = jnp.einsum("gqk,gqh->gkh", softmax_low.astype(jnp.float32), negated, precision=lax.Precision.HIGHEST)
    inner_sum = jnp.sum(softmax_out * grad_probs, axis=-1, keepdims=True)
    grad_scores = (softmax_out * (grad_probs - inner_sum) * scale_factor).astype(jnp.bfloat16)
    scores_wide = grad_scores.astype(jnp.float32)
    grad_queries = jnp.einsum("gqk,gkh->gqh", scores_wide, keys_wide, precision=lax.Precision.HIGHEST) + grad_moved.astype(jnp.float32)
    grad_keys = grad_keys + jnp.einsum("gqk,gqh->gkh", scores_wide, queries.astype(jnp.float32), precision=lax.Precision.HIGHEST)
    return grad_queries, grad_keys


def replica(nodes, cotangent, live, partner_first, partner_size, edge_src, edge_dst, w_edge1, b_edge, w_edge2, w_node1, b_node, w_node2):
    granules, block_rows, state_width = nodes.shape
    node_rows = nodes.reshape(-1, state_width)
    total_rows = node_rows.shape[0]
    positions = jnp.arange(block_rows, dtype=jnp.int32)
    row_mask = (positions[None, :] < live[:, None]).reshape(-1, 1)
    offsets = (jnp.arange(edge_src.shape[0], dtype=jnp.int32) // E_DEV) * (NB * block_rows)
    sources = (edge_src + offsets).astype(jnp.int32)
    targets = (edge_dst + offsets).astype(jnp.int32)

    pre_target = (jnp.dot(node_rows, w_edge1[:state_width], preferred_element_type=jnp.float32) + b_edge).astype(jnp.bfloat16)
    pre_source = jnp.dot(node_rows, w_edge1[state_width:], preferred_element_type=jnp.float32).astype(jnp.bfloat16)
    summed = pre_target[targets].astype(jnp.float32) + pre_source[sources].astype(jnp.float32)
    gathered = jax.ops.segment_sum(jax.nn.silu(summed), targets, num_segments=total_rows).astype(jnp.bfloat16)
    message = jnp.dot(gathered, w_edge2, preferred_element_type=jnp.float32).astype(jnp.bfloat16)

    key_index = jnp.minimum(partner_first[:, None] + jnp.arange(GMAX, dtype=jnp.int32)[None, :], granules - 1).astype(jnp.int32)
    size_mask = jnp.arange(GMAX, dtype=jnp.int32)[None, :] < partner_size[:, None]
    key_mask = (size_mask[:, :, None] & (positions[None, None, :] < live[key_index][:, :, None])).reshape(granules, GMAX * block_rows)
    key_rows = nodes[key_index].reshape(granules, GMAX * block_rows, state_width)
    moved_rows, softmax_out, softmax_low = attend(nodes, key_rows, key_mask)
    moved_flat = moved_rows.reshape(-1, state_width)

    hidden_pre = (jnp.dot(node_rows, w_node1[:state_width], preferred_element_type=jnp.float32)
                  + jnp.dot(message, w_node1[state_width:2 * state_width], preferred_element_type=jnp.float32)
                  + jnp.dot(moved_flat, w_node1[2 * state_width:], preferred_element_type=jnp.float32) + b_node)
    active = jax.nn.silu(hidden_pre).astype(jnp.bfloat16)
    updated = jnp.where(row_mask, node_rows.astype(jnp.float32) + jnp.dot(active, w_node2, preferred_element_type=jnp.float32), 0.0).astype(jnp.bfloat16)

    grad_out = jnp.where(row_mask, cotangent.reshape(-1, state_width), jnp.zeros((), jnp.bfloat16)).astype(jnp.bfloat16)
    g_node2 = jnp.dot(active.T, grad_out, preferred_element_type=jnp.float32)
    grad_hidden = (jnp.dot(grad_out, w_node2.T, preferred_element_type=jnp.float32) * silu_slope(hidden_pre)).astype(jnp.bfloat16)
    g_node1 = jnp.concatenate([jnp.dot(node_rows.T, grad_hidden, preferred_element_type=jnp.float32),
                               jnp.dot(message.T, grad_hidden, preferred_element_type=jnp.float32),
                               jnp.dot(moved_flat.T, grad_hidden, preferred_element_type=jnp.float32)], axis=0)
    g_bnode = jnp.sum(grad_hidden.astype(jnp.float32), axis=0)
    grad_rows = grad_out.astype(jnp.float32) + jnp.dot(grad_hidden, w_node1[:state_width].T, preferred_element_type=jnp.float32)
    grad_message = jnp.dot(grad_hidden, w_node1[state_width:2 * state_width].T, preferred_element_type=jnp.float32).astype(jnp.bfloat16)
    grad_moved = jnp.dot(grad_hidden, w_node1[2 * state_width:].T, preferred_element_type=jnp.float32).astype(jnp.bfloat16)

    grad_queries, grad_keys = attend_back(nodes, key_rows, softmax_out, softmax_low, grad_moved.reshape(granules, block_rows, state_width))
    attention_grad = grad_queries.at[key_index.reshape(-1)].add(grad_keys.reshape(granules * GMAX, block_rows, state_width))

    g_edge2 = jnp.dot(gathered.T, grad_message, preferred_element_type=jnp.float32)
    grad_gathered = jnp.dot(grad_message, w_edge2.T, preferred_element_type=jnp.float32).astype(jnp.bfloat16)
    edge_grad = grad_gathered[targets].astype(jnp.float32) * silu_slope(summed)
    grad_target = jax.ops.segment_sum(edge_grad, targets, num_segments=total_rows).astype(jnp.bfloat16)
    grad_source = jax.ops.segment_sum(edge_grad, sources, num_segments=total_rows).astype(jnp.bfloat16)
    g_edge1 = jnp.concatenate([jnp.dot(node_rows.T, grad_target, preferred_element_type=jnp.float32),
                               jnp.dot(node_rows.T, grad_source, preferred_element_type=jnp.float32)], axis=0)
    g_bedge = jnp.sum(grad_target.astype(jnp.float32), axis=0)
    grad_rows = (grad_rows + attention_grad.reshape(-1, state_width)
                 + jnp.dot(grad_target, w_edge1[:state_width].T, preferred_element_type=jnp.float32)
                 + jnp.dot(grad_source, w_edge1[state_width:].T, preferred_element_type=jnp.float32))
    d_nodes = jnp.where(row_mask, grad_rows, 0.0).astype(jnp.bfloat16)
    return (updated.reshape(granules, block_rows, state_width), d_nodes.reshape(granules, block_rows, state_width),
            g_edge1, g_bedge, g_edge2, g_node1, g_bnode, g_node2)


def reference(nodes, cotangent, live, partner_first, partner_size, edge_src, edge_dst, w_edge1, b_edge, w_edge2, w_node1, b_node, w_node2):
    def one_replica(inputs):
        return replica(inputs[0], inputs[1], inputs[2], inputs[3], inputs[4], inputs[5], inputs[6],
                       w_edge1, b_edge, w_edge2, w_node1, b_node, w_node2)

    results = lax.map(one_replica, (nodes, cotangent, live, partner_first, partner_size, edge_src, edge_dst))
    scale_factor = (N_REP * N_GRAPH * NB * BLK) ** -0.5
    grads = tuple(jnp.sum(item, axis=0) * scale_factor for item in results[2:])
    return (results[0], results[1], grads[0], grads[1], grads[2], grads[3], grads[4], grads[5])
```

```python
import functools

import jax
import jax.numpy as jnp
from jax import lax
from jax.experimental import pallas as pl
from jax.experimental.pallas import tpu as pltpu
from jax.sharding import PartitionSpec as P

GMAX = 2
LANES = 128
F32 = jnp.float32
BF16 = jnp.bfloat16


def dot_nn(a, b):
    return lax.dot_general(a, b, (((1,), (0,)), ((), ())), preferred_element_type=F32)


def dot_nt(a, b):
    return lax.dot_general(a, b, (((1,), (1,)), ((), ())), preferred_element_type=F32)


def dot_tn(a, b):
    return lax.dot_general(a, b, (((0,), (0,)), ((), ())), preferred_element_type=F32)


def sigmoid(v):
    return 1.0 / (1.0 + jnp.exp(-v))


def silu_slope(v, s):
    return s * (1.0 + v * (1.0 - s))


def round_up(value, unit):
    return -(-value // unit) * unit


def send(src, dst, send_sem, recv_sem, graph, rep):
    return pltpu.make_async_remote_copy(
        src_ref=src,
        dst_ref=dst,
        send_sem=send_sem,
        recv_sem=recv_sem,
        device_id={"graph": graph, "rep": rep},
        device_id_type=pl.DeviceIdType.MESH,
    )


class Group:
    def __init__(self, n_graph, n_rep, me, rep, plane_first, refs):
        self.n, self.r, self.me, self.rep = n_graph, n_rep, me, rep
        (self.full, self.r1, self.b, self.r2, self.got,
         self.s1, self.v1, self.s2, self.v2, self.s3, self.v3) = refs
        self.plane_first = plane_first
        self.chips = n_graph // 2
        self.core = lax.rem(me, 2)
        self.chip = lax.div(me, 2)
        self.ch = self.full.shape[1] // self.chips
        self.sends = []
        self.firsts = []

    def go(self, copy):
        copy.start()
        self.sends.append(copy)
        return copy

    def rows(self, q):
        return pl.ds(pl.multiple_of(q * self.ch, 16), self.ch)

    def over_plane(self, source, landing, s, v):
        copies = []
        for d in range(1, self.chips):
            q = lax.rem(self.chip + d, self.chips)
            copies.append(self.go(send(source(q), landing.at[d], s.at[d], v.at[d],
                                       q * 2 + self.core, self.rep)))
        return copies

    def over_rep(self, source, landing, s, v, at=0):
        copies = []
        for d in range(1, self.r):
            z = lax.rem(self.rep + d, self.r)
            copies.append(self.go(send(source(z), landing(d), s.at[at + d], v.at[at + d], self.me, z)))
        return copies

    def first_plane(self):
        self.firsts = self.over_plane(lambda q: self.full.at[:, self.rows(q), :], self.r1, self.s1, self.v1)

    def first_rep(self, part, start, stop):
        self.firsts += self.over_rep(lambda z: self.full.at[z, start:stop],
                                     lambda d: self.r1.at[d, start:stop], self.s1, self.v1, part * self.r)

    def second(self):
        for copy in self.firsts:
            copy.wait_recv()
        if self.plane_first:
            total = self.full[:, self.rows(self.chip), :].astype(F32)
            count = self.chips
        else:
            total = self.full[self.rep].astype(F32)
            count = self.r
        for d in range(1, count):
            total = total + self.r1[d].astype(F32)
        self.b[...] = total.astype(BF16)
        if self.plane_first:
            self.seconds = self.over_rep(lambda z: self.b.at[z], lambda d: self.r2.at[d], self.s2, self.v2)
        else:
            self.seconds = self.over_plane(lambda q: self.b.at[self.rows(q)], self.r2, self.s2, self.v2)

    def gather(self):
        if self.plane_first:
            total = self.b[self.rep].astype(F32)
            count = self.r
        else:
            total = self.b[self.rows(self.chip), :].astype(F32)
            count = self.chips
        for copy in self.seconds:
            copy.wait_recv()
        for d in range(1, count):
            total = total + self.r2[d].astype(F32)
        place = self.core * self.chips + self.chip
        self.got[place] = total.astype(BF16)
        self.thirds = []
        for d in range(1, self.chips):
            to = lax.rem(self.chip + d, self.chips) * 2 + self.core
            frm = self.core * self.chips + lax.rem(self.chip + self.chips - d, self.chips)
            self.go(send(self.got.at[place], self.got.at[place], self.s3.at[d], self.v3.at[d], to, self.rep))
            self.thirds.append(send(self.got.at[frm], self.got.at[frm], self.s3.at[d], self.v3.at[d],
                                    to, self.rep))

    def swap(self):
        for copy in self.thirds:
            copy.wait_recv()
        other = 1 - self.core
        mine = self.got.at[pl.ds(self.core * self.chips, self.chips)]
        theirs = self.got.at[pl.ds(other * self.chips, self.chips)]
        to = self.chip * 2 + other
        self.go(send(mine, mine, self.s3.at[0], self.v3.at[0], to, self.rep))
        self.last = send(theirs, theirs, self.s3.at[0], self.v3.at[0], to, self.rep)

    def finish(self, out):
        self.last.wait_recv()
        out[...] = self.got[...].reshape(self.n * self.ch, LANES)

    def drain(self):
        for copy in self.sends:
            copy.wait_send()


def put_grad(full, offset, grad, n_rep):
    share = grad.shape[0] // n_rep
    low = grad.astype(BF16)
    for j in range(grad.shape[1] // LANES):
        full[:, offset + j * share : offset + (j + 1) * share, :] = low[
            :, j * LANES : (j + 1) * LANES
        ].reshape(n_rep, share, LANES)


def half_rows(shape, n_rep):
    return shape[0] // n_rep * (shape[1] // 2 // LANES)


def take_grad(flat, offset, out, scale):
    share = out.shape[0]
    panels = out.shape[1] // 2 // LANES
    rows = flat.shape[0] // 2
    for c in range(2):
        for j in range(panels):
            at = c * rows + offset + j * share
            col = (c * panels + j) * LANES
            out[:, col : col + LANES] = flat[at : at + share].astype(F32) * scale


def kernel(
    n_graph, n_rep,
    nodes, live, partner, psize, src_ref, dst_ref,
    cot_in, we1_in, be_in, we2_in, wn1_in, bn_in, wn2_in,
    updated_out, dnodes_out, flat_a, flat_b, flat_c, bias_out,
    cot, we1, be, we2, wn1, bn, wn2,
    outgoing, arrived, livebox, livefrom, keygrad, backsend, back, inv,
    msg_f, moved_f, gh_f, act_f, go_f, gat_f, gm_f, gts_f,
    nodes_s, msg_s, moved_s, gh_s, act_s, go_s, gat_s, gm_s, gts_s,
    bias_f, bias_g, bias_m, bias_r,
    load_sem, x_send, x_recv, l_send, l_recv, b_send, b_recv, sib_send, sib_recv,
    c_send, c_recv, d_send, d_recv,
    *group_refs,
):
    me = lax.axis_index("graph")
    rep = lax.axis_index("rep")
    core = lax.rem(me, 2)
    other = 1 - core
    sibling = me + other - core
    G, B, H = nodes.shape
    R = G * B
    half = G // 2
    E = src_ref.shape[1]
    FM = wn1.shape[1]
    per = len(group_refs) // 3
    ga = Group(n_graph, n_rep, me, rep, True, group_refs[:per])
    gb = Group(n_graph, n_rep, me, rep, True, group_refs[per : 2 * per])
    gc = Group(n_graph, n_rep, me, rep, False, group_refs[2 * per :])

    barrier = pltpu.get_barrier_semaphore()
    for d in range(1, n_graph):
        pl.semaphore_signal(barrier, inc=1, device_id={"graph": lax.rem(me + d, n_graph), "rep": rep},
                            device_id_type=pl.DeviceIdType.MESH)
    for d in range(1, n_rep):
        pl.semaphore_signal(barrier, inc=1, device_id={"graph": me, "rep": lax.rem(rep + d, n_rep)},
                            device_id_type=pl.DeviceIdType.MESH)
    loads = []
    pairs = ((we1_in, we1), (be_in, be), (we2_in, we2), (wn1_in, wn1), (bn_in, bn), (cot_in, cot), (wn2_in, wn2))
    for i, (a, b) in enumerate(pairs):
        copy = pltpu.make_async_copy(a, b, load_sem.at[i])
        copy.start()
        loads.append(copy)

    owner = [lax.div(partner[0, g], G) for g in range(G)]
    for g in range(G):
        livebox[g : g + 1, :] = jnp.full((1, LANES), live[0, g].astype(F32))
    livefrom[me] = livebox[...]

    def build(p):
        for h in range(2):
            first = jnp.int32(0)
            count = jnp.int32(0)
            for g in reversed(range(h * half, (h + 1) * half)):
                hit = owner[g] == p
                first = jnp.where(hit, g, first)
                count = count + jnp.where(hit, 1, 0)
            inv[0, p * 2 + h] = first
            inv[1, p * 2 + h] = count
            outgoing[p, h * GMAX * B : h * GMAX * B + B, :] = nodes[first]
            outgoing[p, h * GMAX * B + B : (h + 1) * GMAX * B, :] = nodes[jnp.minimum(first + 1, G - 1)]

    pl.semaphore_wait(barrier, n_graph + n_rep - 2)

    sends = []
    live_waits = []
    for d in range(1, n_graph):
        to = lax.rem(me + d, n_graph)
        frm = lax.rem(me + n_graph - d, n_graph)
        copy = send(livebox, livefrom.at[me], l_send.at[d], l_recv.at[d], to, rep)
        copy.start()
        sends.append(copy)
        live_waits.append(send(livebox, livefrom.at[frm], l_send.at[d], l_recv.at[d], to, rep))

    def ship(d, carry):
        to = lax.rem(me + d, n_graph)
        build(to)
        send(outgoing.at[to], arrived.at[me], x_send.at[d], x_recv.at[d], to, rep).start()
        return carry

    lax.fori_loop(1, n_graph, ship, 0)
    key_waits = []
    for d in range(1, n_graph):
        to = lax.rem(me + d, n_graph)
        frm = lax.rem(me + n_graph - d, n_graph)
        sends.append(send(outgoing.at[to], arrived.at[me], x_send.at[d], x_recv.at[d], to, rep))
        key_waits.append(send(outgoing.at[to], arrived.at[frm], x_send.at[d], x_recv.at[d], to, rep))
    build(me)
    arrived[me] = outgoing[me]

    def share(i, src, dst):
        copy = send(src, dst, sib_send.at[i], sib_recv.at[i], sibling, rep)
        copy.start()
        sends.append(copy)
        return copy

    share_nodes = share(0, nodes, nodes_s)

    rows = nodes[...].reshape(R, H)
    row_ids = lax.broadcasted_iota(jnp.int32, (R, E), 0)
    hot = jnp.concatenate(
        [
            jnp.where(row_ids == dst_ref[...], 1.0, 0.0).astype(BF16),
            jnp.where(row_ids == src_ref[...], 1.0, 0.0).astype(BF16),
        ],
        axis=0,
    )
    loads[0].wait()
    loads[1].wait()
    pre = jnp.concatenate(
        [
            (dot_nn(rows, we1[:H]) + be[...]).astype(BF16),
            dot_nn(rows, we1[H:]).astype(BF16),
        ],
        axis=0,
    )
    summed = dot_tn(hot, pre)
    edge_sig = sigmoid(summed)
    gathered = dot_nn(hot[:R], (summed * edge_sig).astype(BF16)).astype(BF16)
    gat_f[...] = gathered
    share_gat = share(1, gat_f, gat_s)
    loads[2].wait()
    message = dot_nn(gathered, we2[...]).astype(BF16)
    msg_f[...] = message
    share_msg = share(2, msg_f, msg_s)
    loads[3].wait()
    loads[4].wait()
    hidden_pre = dot_nn(rows, wn1[:H]) + dot_nn(message, wn1[H : 2 * H]) + bn[...]
    position = lax.broadcasted_iota(jnp.int32, (B, H), 0)
    mask = jnp.concatenate(
        [jnp.where(position < live[0, g], 1.0, 0.0) for g in range(G)], axis=0
    ) > 0.5
    loads[5].wait()
    loads[6].wait()
    grad_out = jnp.where(mask, cot[...].reshape(R, H).astype(F32), 0.0).astype(BF16)
    for c in range(2):
        go_f[c] = grad_out[:, c * (H // 2) : (c + 1) * (H // 2)]
    share_go = share(3, go_f.at[other], go_s)
    back_hidden = dot_nt(grad_out, wn2[...])

    for copy in live_waits + key_waits:
        copy.wait_recv()
    scale = H ** (-0.5)

    def keys_of(g):
        off = GMAX * B if g < half else 0
        return arrived[owner[g], off : off + GMAX * B, :]

    def block(values, g):
        return values[g * B : (g + 1) * B]

    lane = lax.broadcasted_iota(jnp.int32, (1, LANES), 1).astype(F32)
    score_list, bound_list = [], []
    for g in range(G):
        score_list.append(dot_nt(block(rows, g), keys_of(g)))
        at = partner[0, g] - owner[g] * G
        one = livefrom[owner[g], pl.ds(at, 1), :]
        two = livefrom[owner[g], pl.ds(jnp.minimum(at + 1, G - 1), 1), :]
        two = two * jnp.where(psize[0, g] > 1, 1.0, 0.0)
        bound = jnp.where(lane < B, one, B + two) - lane
        bound_list.append(jnp.broadcast_to(bound[:, : GMAX * B], (B, GMAX * B)))
    scores = jnp.concatenate(score_list, axis=0) * scale
    scores = jnp.where(jnp.concatenate(bound_list, axis=0) > 0.5, scores, -jnp.inf)
    powers = jnp.exp(scores - jnp.max(scores, axis=-1, keepdims=True))
    probs = powers / jnp.sum(powers, axis=-1, keepdims=True)
    low = probs.astype(BF16)
    context = jnp.concatenate([dot_nn(block(low, g), keys_of(g)) for g in range(G)], axis=0)
    moved = (rows.astype(F32) - context).astype(BF16)
    moved_f[...] = moved
    share_moved = share(4, moved_f, moved_s)

    hidden_pre = hidden_pre + dot_nn(moved, wn1[2 * H :])
    sig = sigmoid(hidden_pre)
    grad_hidden = (back_hidden * silu_slope(hidden_pre, sig)).astype(BF16)
    for c in range(2):
        gh_f[c] = grad_hidden[:, c * (FM // 2) : (c + 1) * (FM // 2)]
    share_gh = share(5, gh_f.at[other], gh_s)
    active = (hidden_pre * sig).astype(BF16)
    act_f[...] = active
    share_act = share(6, act_f, act_s)

    grad_message = dot_nt(grad_hidden, wn1[H : 2 * H]).astype(BF16)
    for c in range(2):
        gm_f[c] = grad_message[:, c * (H // 2) : (c + 1) * (H // 2)]
    share_gm = share(7, gm_f.at[other], gm_s)
    grad_gathered = dot_nt(grad_message, we2[...]).astype(BF16)
    edge_grad = (dot_tn(hot[:R], grad_gathered) * silu_slope(summed, edge_sig)).astype(BF16)
    both = dot_nn(hot, edge_grad).astype(BF16)
    for c in range(2):
        gts_f[c] = both[:, c * (FM // 2) : (c + 1) * (FM // 2)]
    share_gts = share(8, gts_f.at[other], gts_s)
    grad_target, grad_source = both[:R], both[R:]

    def two_cores(mine, theirs):
        return jnp.concatenate([mine, theirs], axis=0)

    for copy in (share_nodes, share_msg, share_moved, share_gh):
        copy.wait_recv()
    rows2 = two_cores(rows, nodes_s[...].reshape(R, H))
    gh2 = two_cores(gh_f[core], gh_s[...])
    pieces = jnp.concatenate(
        [dot_tn(rows2, gh2), dot_tn(two_cores(message, msg_s[...]), gh2),
         dot_tn(two_cores(moved, moved_s[...]), gh2)],
        axis=0,
    )
    put_grad(ga.full, 0, pieces, n_rep)
    ga.first_plane()

    for copy in (share_go, share_act):
        copy.wait_recv()
    piece = dot_tn(two_cores(active, act_s[...]), two_cores(go_f[core], go_s[...]))
    put_grad(gc.full, 0, piece, n_rep)
    cut = piece.shape[0] // n_rep * (piece.shape[1] // LANES)
    gc.first_rep(0, 0, cut)

    for copy in (share_gat, share_gm):
        copy.wait_recv()
    piece = dot_tn(two_cores(gathered, gat_s[...]), two_cores(gm_f[core], gm_s[...]))
    put_grad(gc.full, cut, piece, n_rep)
    gc.first_rep(1, cut, gc.full.shape[1])

    share_gts.wait_recv()
    mine, theirs = gts_f[core], gts_s[...]
    pieces = jnp.concatenate(
        [dot_tn(rows2, two_cores(mine[:R], theirs[:R])), dot_tn(rows2, two_cores(mine[R:], theirs[R:]))],
        axis=0,
    )
    put_grad(gb.full, 0, pieces, n_rep)
    gb.first_plane()

    width = FM // n_rep
    sums = (jnp.sum(grad_hidden.astype(F32), axis=0, keepdims=True),
            jnp.sum(grad_target.astype(F32), axis=0, keepdims=True))
    for i in range(2):
        for z in range(n_rep):
            row = sums[i][:, z * width : (z + 1) * width]
            if width < LANES:
                row = jnp.concatenate([row, jnp.zeros((1, LANES - width), F32)], axis=1)
            bias_f[i * n_rep + z : i * n_rep + z + 1, :] = row
    bias_g[me] = bias_f[...]
    bias_waits = []
    for d in range(1, n_graph):
        to = lax.rem(me + d, n_graph)
        frm = lax.rem(me + n_graph - d, n_graph)
        copy = send(bias_f, bias_g.at[me], c_send.at[d], c_recv.at[d], to, rep)
        copy.start()
        sends.append(copy)
        bias_waits.append(send(bias_f, bias_g.at[frm], c_send.at[d], c_recv.at[d], to, rep))

    grad_moved = dot_nt(grad_hidden, wn1[2 * H :]).astype(BF16)
    negated = -grad_moved
    grad_probs = jnp.concatenate(
        [dot_nt(block(negated, g), keys_of(g)) for g in range(G)], axis=0
    )
    inner = jnp.sum(probs * grad_probs, axis=-1, keepdims=True)
    grad_scores = (probs * (grad_probs - inner) * scale).astype(BF16)
    for g in range(G):
        left = jnp.concatenate([block(low, g), block(grad_scores, g)], axis=0)
        right = jnp.concatenate([block(negated, g), block(rows, g)], axis=0)
        keygrad[g] = dot_tn(left, right)

    def ship_back(d, carry):
        to = lax.rem(me + d, n_graph)
        for h in range(2):
            first = inv[0, to * 2 + h]
            count = inv[1, to * 2 + h]
            one = jnp.where(count > 0, 1.0, 0.0)
            two = jnp.where(count > 1, 1.0, 0.0)
            total = keygrad[first] * one + keygrad[jnp.minimum(first + 1, G - 1)] * two
            backsend[to, (1 - h) * GMAX : (2 - h) * GMAX] = total.astype(BF16).reshape(GMAX, B, H)
        return carry

    lax.fori_loop(0, n_graph, ship_back, 0)
    back[me] = backsend[me]
    back_waits = []
    for d in range(1, n_graph):
        to = lax.rem(me + d, n_graph)
        frm = lax.rem(me + n_graph - d, n_graph)
        copy = send(backsend.at[to], back.at[me], b_send.at[d], b_recv.at[d], to, rep)
        copy.start()
        sends.append(copy)
        back_waits.append(send(backsend.at[to], back.at[frm], b_send.at[d], b_recv.at[d], to, rep))

    updated = jnp.where(mask, rows.astype(F32) + dot_nn(active, wn2[...]), 0.0)
    updated_out[...] = updated.astype(BF16).reshape(G, B, H)
    total = grad_out.astype(F32) + grad_moved.astype(F32)
    total = total + dot_nt(grad_hidden, wn1[:H])
    total = total + dot_nt(grad_target, we1[:H]) + dot_nt(grad_source, we1[H:])
    total = total + jnp.concatenate(
        [dot_nn(block(grad_scores, g), keys_of(g)) for g in range(G)], axis=0
    )

    ga.second()
    for copy in bias_waits:
        copy.wait_recv()
    summed_bias = bias_g[0]
    for i in range(1, n_graph):
        summed_bias = summed_bias + bias_g[i]
    bias_m[...] = summed_bias
    bias_r[rep] = summed_bias
    bias_waits = []
    for d in range(1, n_rep):
        to = lax.rem(rep + d, n_rep)
        frm = lax.rem(rep + n_rep - d, n_rep)
        copy = send(bias_m, bias_r.at[rep], d_send.at[d], d_recv.at[d], me, to)
        copy.start()
        sends.append(copy)
        bias_waits.append(send(bias_m, bias_r.at[frm], d_send.at[d], d_recv.at[d], me, to))
    gc.second()
    gb.second()
    for copy in back_waits:
        copy.wait_recv()
    returned = []
    for g in range(G):
        h = 0 if g < half else 1
        same = partner[0, g] == partner[0, g - 1] if g > 0 else False
        place = jnp.where(same, 1, 0)
        returned.append(back[owner[g], h * GMAX + place])
    total = total + jnp.concatenate(returned, axis=0).astype(F32)
    dnodes_out[...] = jnp.where(mask, total, 0.0).astype(BF16).reshape(G, B, H)
    for copy in bias_waits:
        copy.wait_recv()
    for i in range(2):
        row = bias_r[0, pl.ds(i * n_rep + rep, 1), :]
        for z in range(1, n_rep):
            row = row + bias_r[z, pl.ds(i * n_rep + rep, 1), :]
        bias_out[i : i + 1, :] = row

    ga.gather()
    gb.gather()
    gc.gather()
    ga.swap()
    gb.swap()
    gc.swap()
    ga.finish(flat_a)
    gb.finish(flat_b)
    gc.finish(flat_c)
    for copy in sends:
        copy.wait_send()
    for group in (ga, gb, gc):
        group.drain()


def unpack(
    grad_scale, updated, dnodes, flat_a, flat_b, flat_c, bias,
    updated_out, dnodes_out, oe1, obe, oe2, on1, obn, on2,
):
    updated_out[...] = updated[...]
    dnodes_out[...] = dnodes[...]
    take_grad(flat_a, 0, on1, grad_scale)
    take_grad(flat_b, 0, oe1, grad_scale)
    take_grad(flat_c, 0, on2, grad_scale)
    take_grad(flat_c, on2.shape[0] * (on2.shape[1] // 2 // LANES), oe2, grad_scale)
    obn[...] = bias[0:1, : obn.shape[1]] * grad_scale
    obe[...] = bias[1:2, : obe.shape[1]] * grad_scale


def group_scratch(shapes, n_graph, n_rep, plane_first):
    chips = n_graph // 2
    rows = round_up(sum(half_rows(s, n_rep) for s in shapes), 16 * chips)
    ch = rows // chips
    dma = pltpu.SemaphoreType.DMA
    plane = (chips, n_rep, ch, LANES)
    if plane_first:
        middle = [plane, (n_rep, ch, LANES), (n_rep, ch, LANES)]
        first, second = chips, n_rep
    else:
        middle = [(n_rep, rows, LANES), (rows, LANES), (chips, ch, LANES)]
        first, second = len(shapes) * n_rep, chips
    return [pltpu.VMEM((n_rep, rows, LANES), BF16)] + [pltpu.VMEM(s, BF16) for s in middle] + [
        pltpu.VMEM((n_graph, ch, LANES), BF16),
        dma((first,)), dma((first,)), dma((second,)), dma((second,)), dma((n_graph,)), dma((n_graph,)),
    ]


def on_device(
    n_graph, n_rep,
    nodes, cotangent, live, partner_first, partner_size, edge_src, edge_dst,
    w_edge1, b_edge, w_edge2, w_node1, b_node, w_node2,
):
    _, G, B, H = nodes.shape
    FM = w_edge1.shape[1]
    R = G * B
    dma = pltpu.SemaphoreType.DMA
    vmem = pl.BlockSpec(memory_space=pltpu.VMEM)
    smem = pl.BlockSpec(memory_space=pltpu.SMEM)
    hbm = pl.BlockSpec(memory_space=pl.ANY)
    sds = jax.ShapeDtypeStruct

    def share(shape):
        return sds((shape[0] // n_rep,) + tuple(shape[1:]), F32)

    groups = [
        group_scratch([w_node1.shape], n_graph, n_rep, True),
        group_scratch([w_edge1.shape], n_graph, n_rep, True),
        group_scratch([w_node2.shape, w_edge2.shape], n_graph, n_rep, False),
    ]
    flats = tuple(sds((2 * g[0].shape[1], LANES), BF16) for g in groups)
    weights = [cotangent[0], w_edge1, b_edge.reshape(1, FM), w_edge2, w_node1, b_node.reshape(1, FM), w_node2]

    def wide(*shape):
        return pltpu.VMEM(shape, F32)

    def bf(*shape):
        return pltpu.VMEM(shape, BF16)

    parts = pl.pallas_call(
        functools.partial(kernel, n_graph, n_rep),
        out_shape=(sds((G, B, H), BF16), sds((G, B, H), BF16)) + flats + (sds((2, LANES), F32),),
        in_specs=[vmem, smem, smem, smem, vmem, vmem] + [hbm] * 7,
        out_specs=(vmem,) * 6,
        scratch_shapes=[pltpu.VMEM(w.shape, w.dtype) for w in weights]
        + [
            bf(n_graph, 2 * GMAX * B, H),
            bf(n_graph, 2 * GMAX * B, H),
            wide(G, LANES),
            wide(n_graph, G, LANES),
            wide(G, GMAX * B, H),
            bf(n_graph, 2 * GMAX, B, H),
            bf(n_graph, 2 * GMAX, B, H),
            pltpu.SMEM((2, 2 * n_graph), jnp.int32),
            bf(R, H), bf(R, H), bf(2, R, FM // 2), bf(R, FM), bf(2, R, H // 2), bf(R, FM),
            bf(2, R, H // 2), bf(2, 2 * R, FM // 2),
            bf(G, B, H), bf(R, H), bf(R, H), bf(R, FM // 2), bf(R, FM), bf(R, H // 2), bf(R, FM),
            bf(R, H // 2), bf(2 * R, FM // 2),
            wide(2 * n_rep, LANES), wide(n_graph, 2 * n_rep, LANES), wide(2 * n_rep, LANES),
            wide(n_rep, 2 * n_rep, LANES),
            dma((7,)),
            dma((n_graph,)), dma((n_graph,)), dma((n_graph,)), dma((n_graph,)),
            dma((n_graph,)), dma((n_graph,)), dma((9,)), dma((9,)),
            dma((n_graph,)), dma((n_graph,)), dma((n_rep,)), dma((n_rep,)),
        ]
        + sum(groups, []),
        compiler_params=pltpu.CompilerParams(
            collective_id=0, has_side_effects=True, vmem_limit_bytes=64 * 1000 * 1000
        ),
    )(nodes[0], live, partner_first, partner_size, edge_src, edge_dst, *weights)
    outs = pl.pallas_call(
        functools.partial(unpack, (n_graph * n_rep * G * B) ** (-0.5)),
        out_shape=(
            sds((G, B, H), BF16),
            sds((G, B, H), BF16),
            share(w_edge1.shape),
            sds((1, FM // n_rep), F32),
            share(w_edge2.shape),
            share(w_node1.shape),
            sds((1, FM // n_rep), F32),
            share(w_node2.shape),
        ),
        in_specs=[vmem] * 6,
        out_specs=(vmem,) * 8,
    )(*parts)
    return (
        outs[0][None],
        outs[1][None],
        outs[2],
        outs[3].reshape(-1),
        outs[4],
        outs[5],
        outs[6].reshape(-1),
        outs[7],
    )


def solution(mesh):
    rows = P("rep", "graph", None, None)
    ints = P("rep", "graph")
    return jax.shard_map(
        functools.partial(on_device, mesh.shape["graph"], mesh.shape["rep"]),
        mesh=mesh,
        in_specs=(rows, rows, ints, ints, ints, ints, ints) + (P(),) * 6,
        out_specs=(
            rows,
            rows,
            P("rep", None),
            P("rep"),
            P("rep", None),
            P("rep", None),
            P("rep"),
            P("rep", None),
        ),
        check_vma=False,
    )
```

```python
import functools
import math

import jax
import jax.numpy as jnp
from jax import lax
from jax.experimental import pallas as pl
from jax.experimental.pallas import tpu as pltpu
from jax.sharding import PartitionSpec as P

GMAX = 2
LANES = 128
F32 = jnp.float32
BF16 = jnp.bfloat16


def dot_nn(a, b):
    return lax.dot_general(a, b, (((1,), (0,)), ((), ())), preferred_element_type=F32)


def dot_nt(a, b):
    return lax.dot_general(a, b, (((1,), (1,)), ((), ())), preferred_element_type=F32)


def dot_tn(a, b):
    return lax.dot_general(a, b, (((0,), (0,)), ((), ())), preferred_element_type=F32)


def sigmoid(v):
    return 0.5 * jnp.tanh(0.5 * v) + 0.5


def silu_slope(v, s):
    return s * (1.0 + v * (1.0 - s))


def round_up(value, unit):
    return -(-value // unit) * unit


def send(src, dst, send_sem, recv_sem, graph, rep):
    return pltpu.make_async_remote_copy(
        src_ref=src,
        dst_ref=dst,
        send_sem=send_sem,
        recv_sem=recv_sem,
        device_id={"graph": graph, "rep": rep},
        device_id_type=pl.DeviceIdType.MESH,
    )


class Group:
    def __init__(self, n_graph, n_rep, me, rep, plane_first, refs):
        self.n, self.r, self.me, self.rep = n_graph, n_rep, me, rep
        (self.full, self.r1, self.b, self.r2, self.got,
         self.s1, self.v1, self.s2, self.v2, self.s3, self.v3) = refs
        self.plane_first = plane_first
        self.chips = n_graph // 2
        self.core = lax.rem(me, 2)
        self.chip = lax.div(me, 2)
        self.ch = self.full.shape[1] // self.chips
        self.sends = []
        self.firsts = []

    def go(self, copy):
        copy.start()
        self.sends.append(copy)
        return copy

    def rows(self, q):
        return pl.ds(pl.multiple_of(q * self.ch, 16), self.ch)

    def over_plane(self, source, landing, s, v):
        copies = []
        for d in range(1, self.chips):
            q = lax.rem(self.chip + d, self.chips)
            copies.append(self.go(send(source(q), landing.at[d], s.at[d], v.at[d],
                                       q * 2 + self.core, self.rep)))
        return copies

    def over_rep(self, source, landing, s, v, at=0):
        copies = []
        for d in range(1, self.r):
            z = lax.rem(self.rep + d, self.r)
            copies.append(self.go(send(source(z), landing(d), s.at[at + d], v.at[at + d], self.me, z)))
        return copies

    def first_plane(self):
        self.firsts = self.over_plane(lambda q: self.full.at[:, self.rows(q), :], self.r1, self.s1, self.v1)

    def first_rep(self, part, start, stop):
        self.firsts += self.over_rep(lambda z: self.full.at[z, start:stop],
                                     lambda d: self.r1.at[d, start:stop], self.s1, self.v1, part * self.r)

    def second(self):
        for copy in self.firsts:
            copy.wait_recv()
        if self.plane_first:
            total = self.full[:, self.rows(self.chip), :].astype(F32)
            count = self.chips
        else:
            total = self.full[self.rep].astype(F32)
            count = self.r
        for d in range(1, count):
            total = total + self.r1[d].astype(F32)
        self.b[...] = total.astype(BF16)
        if self.plane_first:
            self.seconds = self.over_rep(lambda z: self.b.at[z], lambda d: self.r2.at[d], self.s2, self.v2)
        else:
            self.seconds = self.over_plane(lambda q: self.b.at[self.rows(q)], self.r2, self.s2, self.v2)

    def gather(self):
        if self.plane_first:
            total = self.b[self.rep].astype(F32)
            count = self.r
        else:
            total = self.b[self.rows(self.chip), :].astype(F32)
            count = self.chips
        for copy in self.seconds:
            copy.wait_recv()
        for d in range(1, count):
            total = total + self.r2[d].astype(F32)
        place = self.core * self.chips + self.chip
        self.got[place] = total.astype(BF16)
        self.thirds = []
        for d in range(1, self.chips):
            to = lax.rem(self.chip + d, self.chips) * 2 + self.core
            frm = self.core * self.chips + lax.rem(self.chip + self.chips - d, self.chips)
            self.go(send(self.got.at[place], self.got.at[place], self.s3.at[d], self.v3.at[d], to, self.rep))
            self.thirds.append(send(self.got.at[frm], self.got.at[frm], self.s3.at[d], self.v3.at[d],
                                    to, self.rep))

    def swap(self):
        for copy in self.thirds:
            copy.wait_recv()
        other = 1 - self.core
        mine = self.got.at[pl.ds(self.core * self.chips, self.chips)]
        theirs = self.got.at[pl.ds(other * self.chips, self.chips)]
        to = self.chip * 2 + other
        self.go(send(mine, mine, self.s3.at[0], self.v3.at[0], to, self.rep))
        self.last = send(theirs, theirs, self.s3.at[0], self.v3.at[0], to, self.rep)

    def finish(self, out):
        self.last.wait_recv()
        out[...] = self.got[...].reshape(self.n * self.ch, LANES)

    def drain(self):
        for copy in self.sends:
            copy.wait_send()


def put_grad(full, offset, grad, n_rep):
    share = grad.shape[0] // n_rep
    low = grad.astype(BF16)
    for j in range(grad.shape[1] // LANES):
        full[:, offset + j * share : offset + (j + 1) * share, :] = low[
            :, j * LANES : (j + 1) * LANES
        ].reshape(n_rep, share, LANES)


def half_rows(shape, n_rep):
    return shape[0] // n_rep * (shape[1] // 2 // LANES)


def take_grad(flat, offset, out, scale):
    share = out.shape[0]
    panels = out.shape[1] // 2 // LANES
    rows = flat.shape[0] // 2
    for c in range(2):
        for j in range(panels):
            at = c * rows + offset + j * share
            col = (c * panels + j) * LANES
            out[:, col : col + LANES] = flat[at : at + share].astype(F32) * scale


def kernel(
    n_graph, n_rep,
    *refs
):
    ins, outs, held, rest = refs[:13], refs[13:19], refs[19:32], refs[32:]
    live, partner, psize, nodes, src_ref, dst_ref, we1, be, we2, wn1, bn, cot, wn2 = held
    updated_out, dnodes_out, flat_a, flat_b, flat_c, bias_out = outs
    (outgoing, arrived_low, arrived_high, livebox, livefrom, keygrad, backsend, back, inv,
     msg_f, moved_f, gh_f, act_f, go_f, gat_f, gm_f, gts_f,
     nodes_s, msg_s, moved_s, gh_s, act_s, go_s, gat_s, gm_s, gts_s,
     nodes_t, msg_t, gat_t,
     bias_f, bias_g, bias_m, bias_r,
     load_sem, x_send, x_recv, l_send, l_recv, b_send, b_recv, sib_send, sib_recv,
     c_send, c_recv, d_send, d_recv) = rest[:46]
    group_refs = rest[46:]
    arrived = (arrived_low, arrived_high)
    me = lax.axis_index("graph")
    rep = lax.axis_index("rep")
    core = lax.rem(me, 2)
    other = 1 - core
    sibling = me + other - core
    G, B, H = nodes.shape
    R = G * B
    half = G // 2
    E = src_ref.shape[1]
    FM = wn1.shape[1]
    per = len(group_refs) // 3
    ga = Group(n_graph, n_rep, me, rep, True, group_refs[:per])
    gb = Group(n_graph, n_rep, me, rep, True, group_refs[per : 2 * per])
    gc = Group(n_graph, n_rep, me, rep, False, group_refs[2 * per :])

    loads = []
    for i, (a, b) in enumerate(zip(ins, held)):
        copy = pltpu.make_async_copy(a, b, load_sem.at[i])
        copy.start()
        loads.append(copy)
    barrier = pltpu.get_barrier_semaphore()
    for d in range(1, n_graph):
        pl.semaphore_signal(barrier, inc=1, device_id={"graph": lax.rem(me + d, n_graph), "rep": rep},
                            device_id_type=pl.DeviceIdType.MESH)
    for d in range(1, n_rep):
        pl.semaphore_signal(barrier, inc=1, device_id={"graph": me, "rep": lax.rem(rep + d, n_rep)},
                            device_id_type=pl.DeviceIdType.MESH)
    for copy in loads[:4]:
        copy.wait()
    owner = [lax.div(partner[0, g], G) for g in range(G)]
    for g in range(G):
        livebox[g : g + 1, :] = jnp.full((1, LANES), live[0, g].astype(F32))
    livefrom[me] = livebox[...]

    def build(p, h):
        first = jnp.int32(0)
        count = jnp.int32(0)
        for g in reversed(range(h * half, (h + 1) * half)):
            hit = owner[g] == p
            first = jnp.where(hit, g, first)
            count = count + jnp.where(hit, 1, 0)
        inv[0, p * 2 + h] = first
        inv[1, p * 2 + h] = count
        outgoing[p, h, :B, :] = nodes[first]
        outgoing[p, h, B:, :] = nodes[jnp.minimum(first + 1, G - 1)]

    pl.semaphore_wait(barrier, n_graph + n_rep - 2)

    sends = []
    live_waits = []
    for d in range(1, n_graph):
        to = lax.rem(me + d, n_graph)
        frm = lax.rem(me + n_graph - d, n_graph)
        copy = send(livebox, livefrom.at[me], l_send.at[d], l_recv.at[d], to, rep)
        copy.start()
        sends.append(copy)
        live_waits.append(send(livebox, livefrom.at[frm], l_send.at[d], l_recv.at[d], to, rep))

    key_waits = []
    for h in range(2):

        def ship(i, carry):
            d = lax.rem(i, n_graph - 1) + 1
            to = lax.rem(me + d, n_graph)
            build(to, h)
            send(outgoing.at[to, h], arrived[h].at[me], x_send.at[h * n_graph + d],
                 x_recv.at[h * n_graph + d], to, rep).start()
            return carry

        lax.fori_loop(1, n_graph, ship, 0)
        waits = []
        for d in range(1, n_graph):
            to = lax.rem(me + d, n_graph)
            frm = lax.rem(me + n_graph - d, n_graph)
            s_sem, r_sem = x_send.at[h * n_graph + d], x_recv.at[h * n_graph + d]
            sends.append(send(outgoing.at[to, h], arrived[h].at[me], s_sem, r_sem, to, rep))
            waits.append(send(outgoing.at[to, h], arrived[h].at[frm], s_sem, r_sem, to, rep))
        key_waits.append(waits)
        build(me, h)
        arrived[h][me] = outgoing[me, h]

    def share(i, src, dst):
        copy = send(src, dst, sib_send.at[i], sib_recv.at[i], sibling, rep)
        copy.start()
        sends.append(copy)
        return copy

    share_nodes = share(0, nodes, nodes_s)

    rows = nodes[...].reshape(R, H)
    loads[4].wait()
    loads[5].wait()
    row_ids = lax.broadcasted_iota(jnp.int32, (R, E), 0)
    hot = jnp.concatenate(
        [
            jnp.where(row_ids == dst_ref[...], 1.0, 0.0).astype(BF16),
            jnp.where(row_ids == src_ref[...], 1.0, 0.0).astype(BF16),
        ],
        axis=0,
    )
    hot_t = hot.T
    loads[6].wait()
    loads[7].wait()
    pre = jnp.concatenate(
        [
            (dot_nn(rows, we1[:H]) + be[...]).astype(BF16),
            dot_nn(rows, we1[H:]).astype(BF16),
        ],
        axis=0,
    )
    summed = dot_nn(hot_t, pre)
    edge_sig = sigmoid(summed)
    gathered = dot_nn(hot[:R], (summed * edge_sig).astype(BF16)).astype(BF16)
    gat_f[...] = gathered
    share_gat = share(1, gat_f, gat_s)
    loads[8].wait()
    message = dot_nn(gathered, we2[...]).astype(BF16)
    msg_f[...] = message
    share_msg = share(2, msg_f, msg_s)
    loads[9].wait()
    loads[10].wait()
    hidden_part = dot_nn(rows, wn1[:H]) + dot_nn(message, wn1[H : 2 * H]) + bn[...]
    position = lax.broadcasted_iota(jnp.int32, (B, H), 0)
    mask = jnp.concatenate(
        [jnp.where(position < live[0, g], 1.0, 0.0) for g in range(G)], axis=0
    ) > 0.5
    loads[11].wait()
    loads[12].wait()
    grad_out = jnp.where(mask, cot[...].reshape(R, H).astype(F32), 0.0).astype(BF16)
    for c in range(2):
        go_f[c] = grad_out[:, c * (H // 2) : (c + 1) * (H // 2)]
    share_go = share(3, go_f.at[other], go_s)
    back_hidden = dot_nt(grad_out, wn2[...])

    def two_cores(mine, theirs):
        return jnp.concatenate([mine, theirs], axis=0)

    for copy in (share_nodes, share_gat, share_msg, share_go):
        copy.wait_recv()
    nodes_t[...] = two_cores(rows, nodes_s[...].reshape(R, H)).T
    msg_t[...] = two_cores(message, msg_s[...]).T
    gat_t[...] = two_cores(gathered, gat_s[...]).T

    scale = H ** (-0.5)
    lane = lax.broadcasted_iota(jnp.int32, (1, LANES), 1).astype(F32)

    def keys_of(g):
        return arrived[1 if g < half else 0][owner[g]]

    def block(values, g):
        return values[g * B : (g + 1) * B]

    def bound_of(g):
        at = partner[0, g] - owner[g] * G
        one = livefrom[owner[g], pl.ds(at, 1), :]
        two = livefrom[owner[g], pl.ds(jnp.minimum(at + 1, G - 1), 1), :]
        two = two * jnp.where(psize[0, g] > 1, 1.0, 0.0)
        bound = jnp.where(lane < B, one, B + two) - lane
        return jnp.broadcast_to(bound[:, : GMAX * B], (B, GMAX * B))

    def attend(p):
        part = range(p * half, (p + 1) * half)
        at, to = p * half * B, (p + 1) * half * B
        scores = jnp.concatenate([dot_nt(block(rows, g), keys_of(g)) for g in part], axis=0) * scale
        bounds = jnp.concatenate([bound_of(g) for g in part], axis=0)
        scores = jnp.where(bounds > 0.5, scores, -jnp.inf)
        powers = jnp.exp(scores - jnp.max(scores, axis=-1, keepdims=True))
        probs = powers / jnp.sum(powers, axis=-1, keepdims=True)
        low = probs.astype(BF16)
        context = jnp.concatenate(
            [dot_nn(low[i * B : (i + 1) * B], keys_of(g)) for i, g in enumerate(part)], axis=0
        )
        moved = (rows[at:to].astype(F32) - context).astype(BF16)
        moved_f[at:to, :] = moved
        hidden_pre = hidden_part[at:to] + dot_nn(moved, wn1[2 * H :])
        sig = sigmoid(hidden_pre)
        grad_hidden = (back_hidden[at:to] * silu_slope(hidden_pre, sig)).astype(BF16)
        for c in range(2):
            gh_f[c, at:to, :] = grad_hidden[:, c * (FM // 2) : (c + 1) * (FM // 2)]
        active = (hidden_pre * sig).astype(BF16)
        act_f[at:to, :] = active
        return probs, low, moved, grad_hidden, active

    def message_back(p, grad_hidden):
        at, to = p * half * B, (p + 1) * half * B
        grad_message = dot_nt(grad_hidden, wn1[H : 2 * H]).astype(BF16)
        for c in range(2):
            gm_f[c, at:to, :] = grad_message[:, c * (H // 2) : (c + 1) * (H // 2)]
        return dot_nt(grad_message, we2[...]).astype(BF16)

    for copy in live_waits + key_waits[0]:
        copy.wait_recv()
    upper = attend(1)
    upper_gathered = message_back(1, upper[3])
    for copy in key_waits[1]:
        copy.wait_recv()
    lower = attend(0)
    share_moved = share(4, moved_f, moved_s)
    share_gh = share(5, gh_f.at[other], gh_s)
    share_act = share(6, act_f, act_s)
    lower_gathered = message_back(0, lower[3])
    share_gm = share(7, gm_f.at[other], gm_s)
    probs, low, moved, grad_hidden, active = (
        jnp.concatenate([a, b], axis=0) for a, b in zip(lower, upper)
    )
    grad_gathered = jnp.concatenate([lower_gathered, upper_gathered], axis=0)
    edge_grad = (dot_nn(hot_t[:, :R], grad_gathered) * silu_slope(summed, edge_sig)).astype(BF16)
    both = dot_nn(hot, edge_grad).astype(BF16)
    for c in range(2):
        gts_f[c] = both[:, c * (FM // 2) : (c + 1) * (FM // 2)]
    share_gts = share(8, gts_f.at[other], gts_s)
    grad_target, grad_source = both[:R], both[R:]

    for copy in (share_moved, share_gh):
        copy.wait_recv()
    gh2 = two_cores(gh_f[core], gh_s[...])
    pieces = jnp.concatenate(
        [dot_nn(nodes_t[...], gh2), dot_nn(msg_t[...], gh2),
         dot_tn(two_cores(moved, moved_s[...]), gh2)],
        axis=0,
    )
    put_grad(ga.full, 0, pieces, n_rep)
    ga.first_plane()

    share_act.wait_recv()
    piece = dot_tn(two_cores(active, act_s[...]), two_cores(go_f[core], go_s[...]))
    put_grad(gc.full, 0, piece, n_rep)
    cut = piece.shape[0] // n_rep * (piece.shape[1] // LANES)
    gc.first_rep(0, 0, cut)

    share_gm.wait_recv()
    piece = dot_nn(gat_t[...], two_cores(gm_f[core], gm_s[...]))
    put_grad(gc.full, cut, piece, n_rep)
    gc.first_rep(1, cut, gc.full.shape[1])

    share_gts.wait_recv()
    mine, theirs = gts_f[core], gts_s[...]
    pieces = jnp.concatenate(
        [dot_nn(nodes_t[...], two_cores(mine[:R], theirs[:R])),
         dot_nn(nodes_t[...], two_cores(mine[R:], theirs[R:]))],
        axis=0,
    )
    put_grad(gb.full, 0, pieces, n_rep)
    gb.first_plane()

    width = FM // n_rep
    sums = (jnp.sum(grad_hidden.astype(F32), axis=0, keepdims=True),
            jnp.sum(grad_target.astype(F32), axis=0, keepdims=True))
    for i in range(2):
        for z in range(n_rep):
            row = sums[i][:, z * width : (z + 1) * width]
            if width < LANES:
                row = jnp.concatenate([row, jnp.zeros((1, LANES - width), F32)], axis=1)
            bias_f[i * n_rep + z : i * n_rep + z + 1, :] = row
    bias_g[me] = bias_f[...]
    bias_waits = []
    for d in range(1, n_graph):
        to = lax.rem(me + d, n_graph)
        frm = lax.rem(me + n_graph - d, n_graph)
        copy = send(bias_f, bias_g.at[me], c_send.at[d], c_recv.at[d], to, rep)
        copy.start()
        sends.append(copy)
        bias_waits.append(send(bias_f, bias_g.at[frm], c_send.at[d], c_recv.at[d], to, rep))

    grad_moved = dot_nt(grad_hidden, wn1[2 * H :]).astype(BF16)
    negated = -grad_moved
    grad_probs = jnp.concatenate(
        [dot_nt(block(negated, g), keys_of(g)) for g in range(G)], axis=0
    )
    inner = jnp.sum(probs * grad_probs, axis=-1, keepdims=True)
    grad_scores = (probs * (grad_probs - inner) * scale).astype(BF16)
    for g in range(G):
        left = jnp.concatenate([block(low, g), block(grad_scores, g)], axis=0)
        right = jnp.concatenate([block(negated, g), block(rows, g)], axis=0)
        keygrad[g] = dot_tn(left, right)

    def ship_back(d, carry):
        to = lax.rem(me + d, n_graph)
        for h in range(2):
            first = inv[0, to * 2 + h]
            count = inv[1, to * 2 + h]
            one = jnp.where(count > 0, 1.0, 0.0)
            two = jnp.where(count > 1, 1.0, 0.0)
            total = keygrad[first] * one + keygrad[jnp.minimum(first + 1, G - 1)] * two
            backsend[to, (1 - h) * GMAX : (2 - h) * GMAX] = total.astype(BF16).reshape(GMAX, B, H)
        return carry

    lax.fori_loop(0, n_graph, ship_back, 0)
    back[me] = backsend[me]

    def start_back(h):
        waits = []
        for d in range(1, n_graph):
            to = lax.rem(me + d, n_graph)
            frm = lax.rem(me + n_graph - d, n_graph)
            part = pl.ds(h * GMAX, GMAX)
            s_sem, r_sem = b_send.at[h * n_graph + d], b_recv.at[h * n_graph + d]
            copy = send(backsend.at[to, part], back.at[me, part], s_sem, r_sem, to, rep)
            copy.start()
            sends.append(copy)
            waits.append(send(backsend.at[to, part], back.at[frm, part], s_sem, r_sem, to, rep))
        return waits

    back_waits = start_back(0)
    updated = jnp.where(mask, rows.astype(F32) + dot_nn(active, wn2[...]), 0.0)
    updated_out[...] = updated.astype(BF16).reshape(G, B, H)
    total = grad_out.astype(F32) + grad_moved.astype(F32)
    total = total + dot_nt(grad_hidden, wn1[:H])
    total = total + dot_nt(grad_target, we1[:H]) + dot_nt(grad_source, we1[H:])
    total = total + jnp.concatenate(
        [dot_nn(block(grad_scores, g), keys_of(g)) for g in range(G)], axis=0
    )

    ga.second()
    for copy in bias_waits:
        copy.wait_recv()
    summed_bias = bias_g[0]
    for i in range(1, n_graph):
        summed_bias = summed_bias + bias_g[i]
    bias_m[...] = summed_bias
    bias_r[rep] = summed_bias
    bias_waits = []
    for d in range(1, n_rep):
        to = lax.rem(rep + d, n_rep)
        frm = lax.rem(rep + n_rep - d, n_rep)
        copy = send(bias_m, bias_r.at[rep], d_send.at[d], d_recv.at[d], me, to)
        copy.start()
        sends.append(copy)
        bias_waits.append(send(bias_m, bias_r.at[frm], d_send.at[d], d_recv.at[d], me, to))
    gc.second()
    back_waits += start_back(1)
    gb.second()
    ga.gather()
    gc.gather()
    gb.gather()
    for copy in back_waits:
        copy.wait_recv()
    returned = []
    for g in range(G):
        h = 0 if g < half else 1
        same = partner[0, g] == partner[0, g - 1] if g > 0 else False
        place = jnp.where(same, 1, 0)
        returned.append(back[owner[g], h * GMAX + place])
    total = total + jnp.concatenate(returned, axis=0).astype(F32)
    dnodes_out[...] = jnp.where(mask, total, 0.0).astype(BF16).reshape(G, B, H)
    for copy in bias_waits:
        copy.wait_recv()
    for i in range(2):
        row = bias_r[0, pl.ds(i * n_rep + rep, 1), :]
        for z in range(1, n_rep):
            row = row + bias_r[z, pl.ds(i * n_rep + rep, 1), :]
        bias_out[i : i + 1, :] = row

    for copy in sends:
        copy.wait_send()
    ga.swap()
    gc.swap()
    gb.swap()
    ga.finish(flat_a)
    gc.finish(flat_c)
    gb.finish(flat_b)
    for group in (ga, gb, gc):
        group.drain()


def unpack(
    grad_scale, updated, dnodes, flat_a, flat_b, flat_c, bias,
    updated_out, dnodes_out, oe1, obe, oe2, on1, obn, on2,
    ve1, vbe, ve2, vn1, vbn, vn2, sem,
):
    copies = []

    def put(src, dst):
        copy = pltpu.make_async_copy(src, dst, sem.at[len(copies)])
        copy.start()
        copies.append(copy)

    put(updated, updated_out)
    put(dnodes, dnodes_out)
    take_grad(flat_a, 0, vn1, grad_scale)
    put(vn1, on1)
    take_grad(flat_b, 0, ve1, grad_scale)
    put(ve1, oe1)
    take_grad(flat_c, 0, vn2, grad_scale)
    put(vn2, on2)
    take_grad(flat_c, on2.shape[0] * (on2.shape[1] // 2 // LANES), ve2, grad_scale)
    put(ve2, oe2)
    vbn[...] = bias[0:1, : vbn.shape[1]] * grad_scale
    put(vbn, obn)
    vbe[...] = bias[1:2, : vbe.shape[1]] * grad_scale
    put(vbe, obe)
    for copy in copies:
        copy.wait()


def group_scratch(shapes, n_graph, n_rep, plane_first):
    chips = n_graph // 2
    rows = round_up(sum(half_rows(s, n_rep) for s in shapes), 16 * chips)
    ch = rows // chips
    dma = pltpu.SemaphoreType.DMA
    plane = (chips, n_rep, ch, LANES)
    if plane_first:
        middle = [plane, (n_rep, ch, LANES), (n_rep, ch, LANES)]
        first, second = chips, n_rep
    else:
        middle = [(n_rep, rows, LANES), (rows, LANES), (chips, ch, LANES)]
        first, second = len(shapes) * n_rep, chips
    return [pltpu.VMEM((n_rep, rows, LANES), BF16)] + [pltpu.VMEM(s, BF16) for s in middle] + [
        pltpu.VMEM((n_graph, ch, LANES), BF16),
        dma((first,)), dma((first,)), dma((second,)), dma((second,)), dma((n_graph,)), dma((n_graph,)),
    ]


def on_device(
    n_graph, n_rep,
    nodes, cotangent, live, partner_first, partner_size, edge_src, edge_dst,
    w_edge1, b_edge, w_edge2, w_node1, b_node, w_node2,
):
    _, G, B, H = nodes.shape
    FM = w_edge1.shape[1]
    R = G * B
    dma = pltpu.SemaphoreType.DMA
    vmem = pl.BlockSpec(memory_space=pltpu.VMEM)
    hbm = pl.BlockSpec(memory_space=pltpu.HBM)
    sds = jax.ShapeDtypeStruct

    def share(shape):
        return sds((shape[0] // n_rep,) + tuple(shape[1:]), F32)

    groups = [
        group_scratch([w_node1.shape], n_graph, n_rep, True),
        group_scratch([w_edge1.shape], n_graph, n_rep, True),
        group_scratch([w_node2.shape, w_edge2.shape], n_graph, n_rep, False),
    ]
    flats = tuple(sds((2 * g[0].shape[1], LANES), BF16) for g in groups)
    ints = [live, partner_first, partner_size]
    arrays = [nodes[0], edge_src, edge_dst, w_edge1, b_edge.reshape(1, FM), w_edge2, w_node1,
              b_node.reshape(1, FM), cotangent[0], w_node2]

    def wide(*shape):
        return pltpu.VMEM(shape, F32)

    def bf(*shape):
        return pltpu.VMEM(shape, BF16)

    scratch = (
        [pltpu.SMEM(w.shape, w.dtype) for w in ints]
        + [pltpu.VMEM(w.shape, w.dtype) for w in arrays]
        + [
            bf(n_graph, 2, GMAX * B, H),
            bf(n_graph, GMAX * B, H),
            bf(n_graph, GMAX * B, H),
            wide(G, LANES),
            wide(n_graph, G, LANES),
            wide(G, GMAX * B, H),
            bf(n_graph, 2 * GMAX, B, H),
            bf(n_graph, 2 * GMAX, B, H),
            pltpu.SMEM((2, 2 * n_graph), jnp.int32),
            bf(R, H), bf(R, H), bf(2, R, FM // 2), bf(R, FM), bf(2, R, H // 2), bf(R, FM),
            bf(2, R, H // 2), bf(2, 2 * R, FM // 2),
            bf(G, B, H), bf(R, H), bf(R, H), bf(R, FM // 2), bf(R, FM), bf(R, H // 2), bf(R, FM),
            bf(R, H // 2), bf(2 * R, FM // 2),
            bf(H, 2 * R), bf(H, 2 * R), bf(FM, 2 * R),
            wide(2 * n_rep, LANES), wide(n_graph, 2 * n_rep, LANES), wide(2 * n_rep, LANES),
            wide(n_rep, 2 * n_rep, LANES),
            dma((13,)),
            dma((2 * n_graph,)), dma((2 * n_graph,)), dma((n_graph,)), dma((n_graph,)),
            dma((2 * n_graph,)), dma((2 * n_graph,)), dma((9,)), dma((9,)),
            dma((n_graph,)), dma((n_graph,)), dma((n_rep,)), dma((n_rep,)),
        ]
        + sum(groups, [])
    )
    held = sum(math.prod(w.shape) * w.dtype.itemsize for w in scratch if w.dtype in (BF16, F32))
    parts = pl.pallas_call(
        functools.partial(kernel, n_graph, n_rep),
        out_shape=(sds((G, B, H), BF16), sds((G, B, H), BF16)) + flats + (sds((2, LANES), F32),),
        in_specs=[hbm] * 13,
        out_specs=(vmem,) * 6,
        scratch_shapes=scratch,
        compiler_params=pltpu.CompilerParams(
            collective_id=0, has_side_effects=True, vmem_limit_bytes=min(2 * held, 64 * 1000 * 1000)
        ),
    )(*[pltpu.with_memory_space_constraint(a, pltpu.HBM) for a in ints + arrays])
    shapes = (
        share(w_edge1.shape),
        sds((1, FM // n_rep), F32),
        share(w_edge2.shape),
        share(w_node1.shape),
        sds((1, FM // n_rep), F32),
        share(w_node2.shape),
    )
    outs = pl.pallas_call(
        functools.partial(unpack, (n_graph * n_rep * G * B) ** (-0.5)),
        out_shape=(sds((G, B, H), BF16), sds((G, B, H), BF16)) + shapes,
        in_specs=[vmem] * 6,
        out_specs=(hbm,) * 8,
        scratch_shapes=[pltpu.VMEM(w.shape, F32) for w in shapes] + [dma((8,))],
        compiler_params=pltpu.CompilerParams(vmem_limit_bytes=16 * 1000 * 1000),
    )(*parts)
    return (
        outs[0][None],
        outs[1][None],
        outs[2],
        outs[3].reshape(-1),
        outs[4],
        outs[5],
        outs[6].reshape(-1),
        outs[7],
    )


def solution(mesh):
    rows = P("rep", "graph", None, None)
    ints = P("rep", "graph")
    return jax.shard_map(
        functools.partial(on_device, mesh.shape["graph"], mesh.shape["rep"]),
        mesh=mesh,
        in_specs=(rows, rows, ints, ints, ints, ints, ints) + (P(),) * 6,
        out_specs=(
            rows,
            rows,
            P("rep", None),
            P("rep"),
            P("rep", None),
            P("rep", None),
            P("rep"),
            P("rep", None),
        ),
        check_vma=False,
    )
```

```python
import functools
import math

import jax
import jax.numpy as jnp
from jax import lax
from jax.experimental import pallas as pl
from jax.experimental.pallas import tpu as pltpu
from jax.sharding import PartitionSpec as P

GMAX = 2
MARK = 64.0
LANES = 128
F32 = jnp.float32
BF16 = jnp.bfloat16


def dot_nn(a, b):
    return lax.dot_general(a, b, (((1,), (0,)), ((), ())), preferred_element_type=F32)


def dot_nt(a, b):
    return lax.dot_general(a, b, (((1,), (1,)), ((), ())), preferred_element_type=F32)


def dot_tn(a, b):
    return lax.dot_general(a, b, (((0,), (0,)), ((), ())), preferred_element_type=F32)


def sigmoid(v):
    return 0.5 * jnp.tanh(0.5 * v) + 0.5


def silu_slope(v, s):
    return s * (1.0 + v * (1.0 - s))


def round_up(value, unit):
    return -(-value // unit) * unit


def send(src, dst, send_sem, recv_sem, graph, rep):
    return pltpu.make_async_remote_copy(
        src_ref=src,
        dst_ref=dst,
        send_sem=send_sem,
        recv_sem=recv_sem,
        device_id={"graph": graph, "rep": rep},
        device_id_type=pl.DeviceIdType.MESH,
    )


class Group:
    def __init__(self, n_graph, n_rep, me, rep, plane_first, refs):
        self.n, self.r, self.me, self.rep = n_graph, n_rep, me, rep
        (self.full, self.r1, self.b, self.r2, self.got,
         self.s1, self.v1, self.s2, self.v2, self.s3, self.v3) = refs
        self.plane_first = plane_first
        self.chips = n_graph // 2
        self.core = lax.rem(me, 2)
        self.chip = lax.div(me, 2)
        self.ch = self.full.shape[1] // self.chips
        self.sends = []
        self.firsts = []

    def go(self, copy):
        copy.start()
        self.sends.append(copy)
        return copy

    def rows(self, q):
        return pl.ds(pl.multiple_of(q * self.ch, 16), self.ch)

    def over_plane(self, source, landing, s, v):
        copies = []
        for d in range(1, self.chips):
            q = lax.rem(self.chip + d, self.chips)
            copies.append(self.go(send(source(q), landing.at[d], s.at[d], v.at[d],
                                       q * 2 + self.core, self.rep)))
        return copies

    def over_rep(self, source, landing, s, v, at=0):
        copies = []
        for d in range(1, self.r):
            z = lax.rem(self.rep + d, self.r)
            copies.append(self.go(send(source(z), landing(d), s.at[at + d], v.at[at + d], self.me, z)))
        return copies

    def first_plane(self):
        self.firsts = self.over_plane(lambda q: self.full.at[:, self.rows(q), :], self.r1, self.s1, self.v1)

    def first_rep(self, part, start, stop):
        self.firsts += self.over_rep(lambda z: self.full.at[z, start:stop],
                                     lambda d: self.r1.at[d, start:stop], self.s1, self.v1, part * self.r)

    def second(self):
        for copy in self.firsts:
            copy.wait_recv()
        if self.plane_first:
            total = self.full[:, self.rows(self.chip), :].astype(F32)
            count = self.chips
        else:
            total = self.full[self.rep].astype(F32)
            count = self.r
        for d in range(1, count):
            total = total + self.r1[d].astype(F32)
        self.b[...] = total.astype(BF16)
        if self.plane_first:
            self.seconds = self.over_rep(lambda z: self.b.at[z], lambda d: self.r2.at[d], self.s2, self.v2)
        else:
            self.seconds = self.over_plane(lambda q: self.b.at[self.rows(q)], self.r2, self.s2, self.v2)

    def gather(self, direct=False):
        if self.plane_first:
            total = self.b[self.rep].astype(F32)
            count = self.r
        else:
            total = self.b[self.rows(self.chip), :].astype(F32)
            count = self.chips
        for copy in self.seconds:
            copy.wait_recv()
        for d in range(1, count):
            total = total + self.r2[d].astype(F32)
        place = self.core * self.chips + self.chip
        self.got[place] = total.astype(BF16)
        self.thirds = []
        if direct:
            for d in range(1, self.n):
                to = lax.rem(self.me + d, self.n)
                frm = lax.rem(self.me + self.n - d, self.n)
                theirs = lax.rem(frm, 2) * self.chips + lax.div(frm, 2)
                self.go(send(self.got.at[place], self.got.at[place], self.s3.at[d], self.v3.at[d], to, self.rep))
                self.thirds.append(send(self.got.at[theirs], self.got.at[theirs], self.s3.at[d], self.v3.at[d],
                                        to, self.rep))
            return
        for d in range(1, self.chips):
            to = lax.rem(self.chip + d, self.chips) * 2 + self.core
            frm = self.core * self.chips + lax.rem(self.chip + self.chips - d, self.chips)
            self.go(send(self.got.at[place], self.got.at[place], self.s3.at[d], self.v3.at[d], to, self.rep))
            self.thirds.append(send(self.got.at[frm], self.got.at[frm], self.s3.at[d], self.v3.at[d],
                                    to, self.rep))

    def swap(self):
        for copy in self.thirds:
            copy.wait_recv()
        other = 1 - self.core
        mine = self.got.at[pl.ds(self.core * self.chips, self.chips)]
        theirs = self.got.at[pl.ds(other * self.chips, self.chips)]
        to = self.chip * 2 + other
        self.go(send(mine, mine, self.s3.at[0], self.v3.at[0], to, self.rep))
        self.last = send(theirs, theirs, self.s3.at[0], self.v3.at[0], to, self.rep)

    def finish(self, out, direct=False):
        for copy in self.thirds if direct else [self.last]:
            copy.wait_recv()
        out[...] = self.got[...].reshape(self.n * self.ch, LANES)

    def drain(self):
        for copy in self.sends:
            copy.wait_send()
        self.sends = []


def put_grad(full, offset, grad, n_rep):
    share = grad.shape[0] // n_rep
    low = grad.astype(BF16)
    for j in range(grad.shape[1] // LANES):
        full[:, offset + j * share : offset + (j + 1) * share, :] = low[
            :, j * LANES : (j + 1) * LANES
        ].reshape(n_rep, share, LANES)


def half_rows(shape, n_rep):
    return shape[0] // n_rep * (shape[1] // 2 // LANES)


def take_grad(flat, offset, out, scale):
    share = out.shape[0]
    panels = out.shape[1] // 2 // LANES
    rows = flat.shape[0] // 2
    for c in range(2):
        for j in range(panels):
            at = c * rows + offset + j * share
            col = (c * panels + j) * LANES
            out[:, col : col + LANES] = flat[at : at + share].astype(F32) * scale


def kernel(
    n_graph, n_rep,
    *refs
):
    ins, outs, held, rest = refs[:12], refs[12:18], refs[18:30], refs[30:]
    live, partner, nodes, src_ref, dst_ref, we1, be, we2, wn1, bn, cot, wn2 = held
    updated_out, dnodes_out, flat_a, flat_b, flat_c, bias_out = outs
    (outgoing, arrived_low, arrived_high, keygrad, backsend, back, inv,
     msg_f, moved_f, gh_f, act_f, go_f, gat_f, gm_f, gts_f,
     nodes_s, msg_s, moved_s, gh_s, act_s, go_s, gat_s, gm_s, gts_s,
     nodes_t, msg_t, gat_t,
     bias_f, bias_g, bias_m, bias_r,
     load_sem, x_send, x_recv, b_send, b_recv, sib_send, sib_recv,
     c_send, c_recv, d_send, d_recv) = rest[:42]
    group_refs = rest[42:]
    arrived = (arrived_low, arrived_high)
    me = lax.axis_index("graph")
    rep = lax.axis_index("rep")
    core = lax.rem(me, 2)
    other = 1 - core
    sibling = me + other - core
    G, B, H = nodes.shape
    R = G * B
    half = G // 2
    E = src_ref.shape[1]
    FM = wn1.shape[1]
    per = len(group_refs) // 3
    ga = Group(n_graph, n_rep, me, rep, True, group_refs[:per])
    gb = Group(n_graph, n_rep, me, rep, True, group_refs[per : 2 * per])
    gc = Group(n_graph, n_rep, me, rep, False, group_refs[2 * per :])

    loads = []
    for i, (a, b) in enumerate(zip(ins, held)):
        copy = pltpu.make_async_copy(a, b, load_sem.at[i])
        copy.start()
        loads.append(copy)
    barrier = pltpu.get_barrier_semaphore()
    for d in range(1, n_graph):
        pl.semaphore_signal(barrier, inc=1, device_id={"graph": lax.rem(me + d, n_graph), "rep": rep},
                            device_id_type=pl.DeviceIdType.MESH)
    for d in range(1, n_rep):
        pl.semaphore_signal(barrier, inc=1, device_id={"graph": me, "rep": lax.rem(rep + d, n_rep)},
                            device_id_type=pl.DeviceIdType.MESH)
    for copy in loads[:3]:
        copy.wait()
    owner = [lax.div(partner[0, g], G) for g in range(G)]
    mark_row = lax.broadcasted_iota(jnp.int32, (B, LANES), 0)
    mark_lane = lax.broadcasted_iota(jnp.int32, (B, LANES), 1)

    def marked(g, count):
        mark = jnp.where(mark_row >= count, jnp.where(mark_lane == 0, MARK, 0.0), 0.0)
        return (nodes[g, :, :LANES].astype(F32) + mark).astype(BF16)

    def build(p, h):
        first = jnp.int32(0)
        count = jnp.int32(0)
        for g in reversed(range(h * half, (h + 1) * half)):
            hit = owner[g] == p
            first = jnp.where(hit, g, first)
            count = count + jnp.where(hit, 1, 0)
        inv[0, p * 2 + h] = first
        inv[1, p * 2 + h] = count
        second = jnp.minimum(first + 1, G - 1)
        outgoing[p, h, :B, :LANES] = marked(first, live[0, first])
        outgoing[p, h, B:, :LANES] = marked(second, jnp.where(count > 1, live[0, second], 0))
        outgoing[p, h, :B, LANES:] = nodes[first, :, LANES:]
        outgoing[p, h, B:, LANES:] = nodes[second, :, LANES:]

    pl.semaphore_wait(barrier, n_graph + n_rep - 2)

    sends = []
    key_waits = []
    for h in range(2):

        def ship(i, carry):
            d = lax.rem(i, n_graph - 1) + 1
            to = lax.rem(me + d, n_graph)
            build(to, h)
            send(outgoing.at[to, h], arrived[h].at[me], x_send.at[h * n_graph + d],
                 x_recv.at[h * n_graph + d], to, rep).start()
            return carry

        lax.fori_loop(1, n_graph, ship, 0)
        waits = []
        for d in range(1, n_graph):
            to = lax.rem(me + d, n_graph)
            frm = lax.rem(me + n_graph - d, n_graph)
            s_sem, r_sem = x_send.at[h * n_graph + d], x_recv.at[h * n_graph + d]
            sends.append(send(outgoing.at[to, h], arrived[h].at[me], s_sem, r_sem, to, rep))
            waits.append(send(outgoing.at[to, h], arrived[h].at[frm], s_sem, r_sem, to, rep))
        key_waits.append(waits)
        build(me, h)
        arrived[h][me] = outgoing[me, h]

    def share(i, src, dst):
        copy = send(src, dst, sib_send.at[i], sib_recv.at[i], sibling, rep)
        copy.start()
        sends.append(copy)
        return copy

    share_nodes = share(0, nodes, nodes_s)

    rows = nodes[...].reshape(R, H)
    loads[3].wait()
    loads[4].wait()
    row_ids = lax.broadcasted_iota(jnp.int32, (R, E), 0)
    hot = jnp.concatenate(
        [
            jnp.where(row_ids == dst_ref[...], 1.0, 0.0).astype(BF16),
            jnp.where(row_ids == src_ref[...], 1.0, 0.0).astype(BF16),
        ],
        axis=0,
    )
    hot_t = hot.T
    loads[5].wait()
    loads[6].wait()
    pre = jnp.concatenate(
        [
            (dot_nn(rows, we1[:H]) + be[...]).astype(BF16),
            dot_nn(rows, we1[H:]).astype(BF16),
        ],
        axis=0,
    )
    summed = dot_nn(hot_t, pre)
    edge_sig = sigmoid(summed)
    gathered = dot_nn(hot[:R], (summed * edge_sig).astype(BF16)).astype(BF16)
    gat_f[...] = gathered
    share_gat = share(1, gat_f, gat_s)
    loads[7].wait()
    message = dot_nn(gathered, we2[...]).astype(BF16)
    msg_f[...] = message
    share_msg = share(2, msg_f, msg_s)
    loads[8].wait()
    loads[9].wait()
    hidden_part = dot_nn(rows, wn1[:H]) + dot_nn(message, wn1[H : 2 * H]) + bn[...]
    position = lax.broadcasted_iota(jnp.int32, (B, H), 0)
    mask = jnp.concatenate(
        [jnp.where(position < live[0, g], 1.0, 0.0) for g in range(G)], axis=0
    ) > 0.5
    loads[10].wait()
    loads[11].wait()
    grad_out = jnp.where(mask, cot[...].reshape(R, H).astype(F32), 0.0).astype(BF16)
    for c in range(2):
        go_f[c] = grad_out[:, c * (H // 2) : (c + 1) * (H // 2)]
    share_go = share(3, go_f.at[other], go_s)
    back_hidden = dot_nt(grad_out, wn2[...])

    def two_cores(mine, theirs):
        return jnp.concatenate([mine, theirs], axis=0)

    for copy in (share_nodes, share_gat, share_msg, share_go):
        copy.wait_recv()
    nodes_t[...] = two_cores(rows, nodes_s[...].reshape(R, H)).T
    msg_t[...] = two_cores(message, msg_s[...]).T
    gat_t[...] = two_cores(gathered, gat_s[...]).T

    scale = H ** (-0.5)
    first_lane = lax.broadcasted_iota(jnp.int32, (16, H), 1) == 0
    pick = jnp.where(first_lane, 1.0, 0.0).astype(BF16)

    def keys_of(g):
        return arrived[1 if g < half else 0][owner[g]]

    def block(values, g):
        return values[g * B : (g + 1) * B]

    def attend(p):
        part = range(p * half, (p + 1) * half)
        at, to = p * half * B, (p + 1) * half * B
        products = [dot_nt(jnp.concatenate([block(rows, g), pick], axis=0), keys_of(g)) for g in part]
        marks = jnp.concatenate([jnp.broadcast_to(v[B : B + 1], (B, GMAX * B)) for v in products], axis=0)
        scores = jnp.concatenate([v[:B] for v in products], axis=0) * scale
        scores = jnp.where(marks < 0.5 * MARK, scores, -jnp.inf)
        powers = jnp.exp(scores - jnp.max(scores, axis=-1, keepdims=True))
        probs = powers / jnp.sum(powers, axis=-1, keepdims=True)
        low = probs.astype(BF16)
        context = jnp.concatenate(
            [dot_nn(low[i * B : (i + 1) * B], keys_of(g)) for i, g in enumerate(part)], axis=0
        )
        moved = (rows[at:to].astype(F32) - context).astype(BF16)
        moved_f[at:to, :] = moved
        hidden_pre = hidden_part[at:to] + dot_nn(moved, wn1[2 * H :])
        sig = sigmoid(hidden_pre)
        grad_hidden = (back_hidden[at:to] * silu_slope(hidden_pre, sig)).astype(BF16)
        for c in range(2):
            gh_f[c, at:to, :] = grad_hidden[:, c * (FM // 2) : (c + 1) * (FM // 2)]
        return probs, low, moved, grad_hidden, hidden_pre, sig

    def activate(p, hidden_pre, sig):
        active = (hidden_pre * sig).astype(BF16)
        act_f[p * half * B : (p + 1) * half * B, :] = active
        return active

    def message_back(p, grad_hidden):
        at, to = p * half * B, (p + 1) * half * B
        grad_message = dot_nt(grad_hidden, wn1[H : 2 * H]).astype(BF16)
        for c in range(2):
            gm_f[c, at:to, :] = grad_message[:, c * (H // 2) : (c + 1) * (H // 2)]
        return dot_nt(grad_message, we2[...]).astype(BF16)

    for copy in key_waits[0]:
        copy.wait_recv()
    upper = attend(1)
    upper_active = activate(1, *upper[4:])
    upper_gathered = message_back(1, upper[3])
    for copy in key_waits[1]:
        copy.wait_recv()
    lower = attend(0)
    share_moved = share(4, moved_f, moved_s)
    share_gh = share(5, gh_f.at[other], gh_s)
    lower_active = activate(0, *lower[4:])
    share_act = share(6, act_f, act_s)
    lower_gathered = message_back(0, lower[3])
    share_gm = share(7, gm_f.at[other], gm_s)
    probs, low, moved, grad_hidden = (
        jnp.concatenate([a, b], axis=0) for a, b in zip(lower[:4], upper[:4])
    )
    active = jnp.concatenate([lower_active, upper_active], axis=0)

    def node_pieces(part, moved_rows, gh):
        return jnp.concatenate(
            [dot_nn(nodes_t[:, part], gh), dot_nn(msg_t[:, part], gh), dot_tn(moved_rows, gh)], axis=0
        )

    mine = node_pieces(slice(0, R), moved, gh_f[core])
    for copy in (share_moved, share_gh):
        copy.wait_recv()
    put_grad(ga.full, 0, mine + node_pieces(slice(R, 2 * R), moved_s[...], gh_s[...]), n_rep)
    ga.first_plane()

    share_act.wait_recv()
    piece = dot_tn(two_cores(active, act_s[...]), two_cores(go_f[core], go_s[...]))
    put_grad(gc.full, 0, piece, n_rep)
    cut = piece.shape[0] // n_rep * (piece.shape[1] // LANES)
    gc.first_rep(0, 0, cut)

    grad_gathered = jnp.concatenate([lower_gathered, upper_gathered], axis=0)
    edge_grad = (dot_nn(hot_t[:, :R], grad_gathered) * silu_slope(summed, edge_sig)).astype(BF16)
    both = dot_nn(hot, edge_grad).astype(BF16)
    for c in range(2):
        gts_f[c] = both[:, c * (FM // 2) : (c + 1) * (FM // 2)]
    share_gts = share(8, gts_f.at[other], gts_s)
    grad_target, grad_source = both[:R], both[R:]

    share_gm.wait_recv()
    piece = dot_nn(gat_t[...], two_cores(gm_f[core], gm_s[...]))
    put_grad(gc.full, cut, piece, n_rep)
    gc.first_rep(1, cut, gc.full.shape[1])

    width = FM // n_rep
    sums = (jnp.sum(grad_hidden.astype(F32), axis=0, keepdims=True),
            jnp.sum(grad_target.astype(F32), axis=0, keepdims=True))
    for i in range(2):
        for z in range(n_rep):
            row = sums[i][:, z * width : (z + 1) * width]
            if width < LANES:
                row = jnp.concatenate([row, jnp.zeros((1, LANES - width), F32)], axis=1)
            bias_f[i * n_rep + z : i * n_rep + z + 1, :] = row
    bias_g[me] = bias_f[...]
    bias_waits = []
    for d in range(1, n_graph):
        to = lax.rem(me + d, n_graph)
        frm = lax.rem(me + n_graph - d, n_graph)
        copy = send(bias_f, bias_g.at[me], c_send.at[d], c_recv.at[d], to, rep)
        copy.start()
        sends.append(copy)
        bias_waits.append(send(bias_f, bias_g.at[frm], c_send.at[d], c_recv.at[d], to, rep))

    share_gts.wait_recv()
    mine, theirs = gts_f[core], gts_s[...]
    pieces = jnp.concatenate(
        [dot_nn(nodes_t[...], two_cores(mine[:R], theirs[:R])),
         dot_nn(nodes_t[...], two_cores(mine[R:], theirs[R:]))],
        axis=0,
    )
    put_grad(gb.full, 0, pieces, n_rep)
    gb.first_plane()

    grad_moved = dot_nt(grad_hidden, wn1[2 * H :]).astype(BF16)
    negated = -grad_moved
    grad_probs = jnp.concatenate(
        [dot_nt(block(negated, g), keys_of(g)) for g in range(G)], axis=0
    )
    inner = jnp.sum(probs * grad_probs, axis=-1, keepdims=True)
    grad_scores = (probs * (grad_probs - inner) * scale).astype(BF16)
    for g in range(G):
        left = jnp.concatenate([block(low, g), block(grad_scores, g)], axis=0)
        right = jnp.concatenate([block(negated, g), block(rows, g)], axis=0)
        keygrad[g] = dot_tn(left, right)

    def ship_back(d, carry):
        to = lax.rem(me + d, n_graph)
        for h in range(2):
            first = inv[0, to * 2 + h]
            count = inv[1, to * 2 + h]
            one = jnp.where(count > 0, 1.0, 0.0)
            two = jnp.where(count > 1, 1.0, 0.0)
            total = keygrad[first] * one + keygrad[jnp.minimum(first + 1, G - 1)] * two
            backsend[to, (1 - h) * GMAX : (2 - h) * GMAX] = total.astype(BF16).reshape(GMAX, B, H)
        return carry

    lax.fori_loop(0, n_graph, ship_back, 0)
    back[me] = backsend[me]

    def start_back(h):
        waits = []
        for d in range(1, n_graph):
            to = lax.rem(me + d, n_graph)
            frm = lax.rem(me + n_graph - d, n_graph)
            part = pl.ds(h * GMAX, GMAX)
            s_sem, r_sem = b_send.at[h * n_graph + d], b_recv.at[h * n_graph + d]
            copy = send(backsend.at[to, part], back.at[me, part], s_sem, r_sem, to, rep)
            copy.start()
            sends.append(copy)
            waits.append(send(backsend.at[to, part], back.at[frm, part], s_sem, r_sem, to, rep))
        return waits

    back_waits = start_back(0)
    updated = jnp.where(mask, rows.astype(F32) + dot_nn(active, wn2[...]), 0.0)
    updated_out[...] = updated.astype(BF16).reshape(G, B, H)
    total = grad_out.astype(F32) + grad_moved.astype(F32)
    total = total + dot_nt(grad_hidden, wn1[:H])
    total = total + dot_nt(grad_target, we1[:H]) + dot_nt(grad_source, we1[H:])
    total = total + jnp.concatenate(
        [dot_nn(block(grad_scores, g), keys_of(g)) for g in range(G)], axis=0
    )

    ga.second()
    for copy in bias_waits:
        copy.wait_recv()
    summed_bias = bias_g[0]
    for i in range(1, n_graph):
        summed_bias = summed_bias + bias_g[i]
    bias_m[...] = summed_bias
    bias_r[rep] = summed_bias
    bias_waits = []
    for d in range(1, n_rep):
        to = lax.rem(rep + d, n_rep)
        frm = lax.rem(rep + n_rep - d, n_rep)
        copy = send(bias_m, bias_r.at[rep], d_send.at[d], d_recv.at[d], me, to)
        copy.start()
        sends.append(copy)
        bias_waits.append(send(bias_m, bias_r.at[frm], d_send.at[d], d_recv.at[d], me, to))
    gc.second()
    back_waits += start_back(1)
    gb.second()
    ga.drain()
    ga.gather()
    gc.drain()
    gc.gather()
    gb.drain()
    gb.gather(direct=True)
    for copy in back_waits:
        copy.wait_recv()
    returned = []
    for g in range(G):
        h = 0 if g < half else 1
        same = partner[0, g] == partner[0, g - 1] if g > 0 else False
        place = jnp.where(same, 1, 0)
        returned.append(back[owner[g], h * GMAX + place])
    total = total + jnp.concatenate(returned, axis=0).astype(F32)
    dnodes_out[...] = jnp.where(mask, total, 0.0).astype(BF16).reshape(G, B, H)
    for copy in bias_waits:
        copy.wait_recv()
    for i in range(2):
        row = bias_r[0, pl.ds(i * n_rep + rep, 1), :]
        for z in range(1, n_rep):
            row = row + bias_r[z, pl.ds(i * n_rep + rep, 1), :]
        bias_out[i : i + 1, :] = row

    for copy in sends:
        copy.wait_send()
    ga.swap()
    gc.swap()
    ga.finish(flat_a)
    gc.finish(flat_c)
    gb.finish(flat_b, direct=True)
    for group in (ga, gb, gc):
        group.drain()


def unpack(
    grad_scale, updated, dnodes, flat_a, flat_b, flat_c, bias,
    updated_out, dnodes_out, oe1, obe, oe2, on1, obn, on2,
    ve1, vbe, ve2, vn1, vbn, vn2, sem,
):
    copies = []

    def put(src, dst):
        copy = pltpu.make_async_copy(src, dst, sem.at[len(copies)])
        copy.start()
        copies.append(copy)

    put(updated, updated_out)
    put(dnodes, dnodes_out)
    take_grad(flat_a, 0, vn1, grad_scale)
    put(vn1, on1)
    take_grad(flat_b, 0, ve1, grad_scale)
    put(ve1, oe1)
    take_grad(flat_c, 0, vn2, grad_scale)
    put(vn2, on2)
    take_grad(flat_c, on2.shape[0] * (on2.shape[1] // 2 // LANES), ve2, grad_scale)
    put(ve2, oe2)
    vbn[...] = bias[0:1, : vbn.shape[1]] * grad_scale
    put(vbn, obn)
    vbe[...] = bias[1:2, : vbe.shape[1]] * grad_scale
    put(vbe, obe)
    for copy in copies:
        copy.wait()


def group_scratch(shapes, n_graph, n_rep, plane_first):
    chips = n_graph // 2
    rows = round_up(sum(half_rows(s, n_rep) for s in shapes), 16 * chips)
    ch = rows // chips
    dma = pltpu.SemaphoreType.DMA
    plane = (chips, n_rep, ch, LANES)
    if plane_first:
        middle = [plane, (n_rep, ch, LANES), (n_rep, ch, LANES)]
        first, second = chips, n_rep
    else:
        middle = [(n_rep, rows, LANES), (rows, LANES), (chips, ch, LANES)]
        first, second = len(shapes) * n_rep, chips
    return [pltpu.VMEM((n_rep, rows, LANES), BF16)] + [pltpu.VMEM(s, BF16) for s in middle] + [
        pltpu.VMEM((n_graph, ch, LANES), BF16),
        dma((first,)), dma((first,)), dma((second,)), dma((second,)), dma((n_graph,)), dma((n_graph,)),
    ]


def on_device(
    n_graph, n_rep,
    nodes, cotangent, live, partner_first, partner_size, edge_src, edge_dst,
    w_edge1, b_edge, w_edge2, w_node1, b_node, w_node2,
):
    _, G, B, H = nodes.shape
    FM = w_edge1.shape[1]
    R = G * B
    dma = pltpu.SemaphoreType.DMA
    vmem = pl.BlockSpec(memory_space=pltpu.VMEM)
    hbm = pl.BlockSpec(memory_space=pltpu.HBM)
    sds = jax.ShapeDtypeStruct

    def share(shape):
        return sds((shape[0] // n_rep,) + tuple(shape[1:]), F32)

    groups = [
        group_scratch([w_node1.shape], n_graph, n_rep, True),
        group_scratch([w_edge1.shape], n_graph, n_rep, True),
        group_scratch([w_node2.shape, w_edge2.shape], n_graph, n_rep, False),
    ]
    flats = tuple(sds((2 * g[0].shape[1], LANES), BF16) for g in groups)
    ints = [live, partner_first]
    arrays = [nodes[0], edge_src, edge_dst, w_edge1, b_edge.reshape(1, FM), w_edge2, w_node1,
              b_node.reshape(1, FM), cotangent[0], w_node2]

    def wide(*shape):
        return pltpu.VMEM(shape, F32)

    def bf(*shape):
        return pltpu.VMEM(shape, BF16)

    scratch = (
        [pltpu.SMEM(w.shape, w.dtype) for w in ints]
        + [pltpu.VMEM(w.shape, w.dtype) for w in arrays]
        + [
            bf(n_graph, 2, GMAX * B, H),
            bf(n_graph, GMAX * B, H),
            bf(n_graph, GMAX * B, H),
            wide(G, GMAX * B, H),
            bf(n_graph, 2 * GMAX, B, H),
            bf(n_graph, 2 * GMAX, B, H),
            pltpu.SMEM((2, 2 * n_graph), jnp.int32),
            bf(R, H), bf(R, H), bf(2, R, FM // 2), bf(R, FM), bf(2, R, H // 2), bf(R, FM),
            bf(2, R, H // 2), bf(2, 2 * R, FM // 2),
            bf(G, B, H), bf(R, H), bf(R, H), bf(R, FM // 2), bf(R, FM), bf(R, H // 2), bf(R, FM),
            bf(R, H // 2), bf(2 * R, FM // 2),
            bf(H, 2 * R), bf(H, 2 * R), bf(FM, 2 * R),
            wide(2 * n_rep, LANES), wide(n_graph, 2 * n_rep, LANES), wide(2 * n_rep, LANES),
            wide(n_rep, 2 * n_rep, LANES),
            dma((12,)),
            dma((2 * n_graph,)), dma((2 * n_graph,)),
            dma((2 * n_graph,)), dma((2 * n_graph,)), dma((9,)), dma((9,)),
            dma((n_graph,)), dma((n_graph,)), dma((n_rep,)), dma((n_rep,)),
        ]
        + sum(groups, [])
    )
    held = sum(math.prod(w.shape) * w.dtype.itemsize for w in scratch if w.dtype in (BF16, F32))
    parts = pl.pallas_call(
        functools.partial(kernel, n_graph, n_rep),
        out_shape=(sds((G, B, H), BF16), sds((G, B, H), BF16)) + flats + (sds((2, LANES), F32),),
        in_specs=[hbm] * 12,
        out_specs=(vmem,) * 6,
        scratch_shapes=scratch,
        compiler_params=pltpu.CompilerParams(
            collective_id=0, has_side_effects=True, vmem_limit_bytes=min(2 * held, 64 * 1000 * 1000)
        ),
    )(*[pltpu.with_memory_space_constraint(a, pltpu.HBM) for a in ints + arrays])
    shapes = (
        share(w_edge1.shape),
        sds((1, FM // n_rep), F32),
        share(w_edge2.shape),
        share(w_node1.shape),
        sds((1, FM // n_rep), F32),
        share(w_node2.shape),
    )
    outs = pl.pallas_call(
        functools.partial(unpack, (n_graph * n_rep * G * B) ** (-0.5)),
        out_shape=(sds((G, B, H), BF16), sds((G, B, H), BF16)) + shapes,
        in_specs=[vmem] * 6,
        out_specs=(hbm,) * 8,
        scratch_shapes=[pltpu.VMEM(w.shape, F32) for w in shapes] + [dma((8,))],
        compiler_params=pltpu.CompilerParams(vmem_limit_bytes=16 * 1000 * 1000),
    )(*parts)
    return (
        outs[0][None],
        outs[1][None],
        outs[2],
        outs[3].reshape(-1),
        outs[4],
        outs[5],
        outs[6].reshape(-1),
        outs[7],
    )


def solution(mesh):
    rows = P("rep", "graph", None, None)
    ints = P("rep", "graph")
    return jax.shard_map(
        functools.partial(on_device, mesh.shape["graph"], mesh.shape["rep"]),
        mesh=mesh,
        in_specs=(rows, rows, ints, ints, ints, ints, ints) + (P(),) * 6,
        out_specs=(
            rows,
            rows,
            P("rep", None),
            P("rep"),
            P("rep", None),
            P("rep", None),
            P("rep"),
            P("rep", None),
        ),
        check_vma=False,
    )
```

```python
import functools
import math

import jax
import jax.numpy as jnp
from jax import lax
from jax.experimental import pallas as pl
from jax.experimental.pallas import tpu as pltpu
from jax.sharding import PartitionSpec as P

GMAX = 2
MARK = 64.0
LANES = 128
F32 = jnp.float32
BF16 = jnp.bfloat16


def dot_nn(a, b):
    return lax.dot_general(a, b, (((1,), (0,)), ((), ())), preferred_element_type=F32)


def dot_nt(a, b):
    return lax.dot_general(a, b, (((1,), (1,)), ((), ())), preferred_element_type=F32)


def dot_tn(a, b):
    return lax.dot_general(a, b, (((0,), (0,)), ((), ())), preferred_element_type=F32)


def sigmoid(v):
    return 0.5 * jnp.tanh(0.5 * v) + 0.5


def silu_slope(v, s):
    return s * (1.0 + v * (1.0 - s))


def round_up(value, unit):
    return -(-value // unit) * unit


def send(src, dst, send_sem, recv_sem, graph, rep):
    return pltpu.make_async_remote_copy(
        src_ref=src,
        dst_ref=dst,
        send_sem=send_sem,
        recv_sem=recv_sem,
        device_id={"graph": graph, "rep": rep},
        device_id_type=pl.DeviceIdType.MESH,
    )


class Group:
    def __init__(self, n_graph, n_rep, me, rep, plane_first, refs):
        self.n, self.r, self.me, self.rep = n_graph, n_rep, me, rep
        (self.full, self.r1, self.b, self.r2, self.got,
         self.s1, self.v1, self.s2, self.v2, self.s3, self.v3) = refs
        self.plane_first = plane_first
        self.chips = n_graph // 2
        self.core = lax.rem(me, 2)
        self.chip = lax.div(me, 2)
        self.ch = self.full.shape[1] // self.chips
        self.sends = []
        self.firsts = []

    def go(self, copy):
        copy.start()
        self.sends.append(copy)
        return copy

    def rows(self, q):
        return pl.ds(pl.multiple_of(q * self.ch, 16), self.ch)

    def over_plane(self, source, landing, s, v):
        copies = []
        for d in range(1, self.chips):
            q = lax.rem(self.chip + d, self.chips)
            copies.append(self.go(send(source(q), landing.at[d], s.at[d], v.at[d],
                                       q * 2 + self.core, self.rep)))
        return copies

    def over_rep(self, source, landing, s, v, at=0):
        copies = []
        for d in range(1, self.r):
            z = lax.rem(self.rep + d, self.r)
            copies.append(self.go(send(source(z), landing(d), s.at[at + d], v.at[at + d], self.me, z)))
        return copies

    def first_plane(self):
        self.firsts = self.over_plane(lambda q: self.full.at[:, self.rows(q), :], self.r1, self.s1, self.v1)

    def first_rep(self, part, start, stop):
        self.firsts += self.over_rep(lambda z: self.full.at[z, start:stop],
                                     lambda d: self.r1.at[d, start:stop], self.s1, self.v1, part * self.r)

    def second(self):
        for copy in self.firsts:
            copy.wait_recv()
        if self.plane_first:
            total = self.full[:, self.rows(self.chip), :].astype(F32)
            count = self.chips
        else:
            total = self.full[self.rep].astype(F32)
            count = self.r
        for d in range(1, count):
            total = total + self.r1[d].astype(F32)
        self.b[...] = total.astype(BF16)
        if self.plane_first:
            self.seconds = self.over_rep(lambda z: self.b.at[z], lambda d: self.r2.at[d], self.s2, self.v2)
        else:
            self.seconds = self.over_plane(lambda q: self.b.at[self.rows(q)], self.r2, self.s2, self.v2)

    def gather(self, direct=False):
        if self.plane_first:
            total = self.b[self.rep].astype(F32)
            count = self.r
        else:
            total = self.b[self.rows(self.chip), :].astype(F32)
            count = self.chips
        for copy in self.seconds:
            copy.wait_recv()
        for d in range(1, count):
            total = total + self.r2[d].astype(F32)
        place = self.core * self.chips + self.chip
        self.got[place] = total.astype(BF16)
        self.thirds = []
        if direct:
            for d in range(1, self.n):
                to = lax.rem(self.me + d, self.n)
                frm = lax.rem(self.me + self.n - d, self.n)
                theirs = lax.rem(frm, 2) * self.chips + lax.div(frm, 2)
                self.go(send(self.got.at[place], self.got.at[place], self.s3.at[d], self.v3.at[d], to, self.rep))
                self.thirds.append(send(self.got.at[theirs], self.got.at[theirs], self.s3.at[d], self.v3.at[d],
                                        to, self.rep))
            return
        for d in range(1, self.chips):
            to = lax.rem(self.chip + d, self.chips) * 2 + self.core
            frm = self.core * self.chips + lax.rem(self.chip + self.chips - d, self.chips)
            self.go(send(self.got.at[place], self.got.at[place], self.s3.at[d], self.v3.at[d], to, self.rep))
            self.thirds.append(send(self.got.at[frm], self.got.at[frm], self.s3.at[d], self.v3.at[d],
                                    to, self.rep))

    def swap(self):
        for copy in self.thirds:
            copy.wait_recv()
        other = 1 - self.core
        mine = self.got.at[pl.ds(self.core * self.chips, self.chips)]
        theirs = self.got.at[pl.ds(other * self.chips, self.chips)]
        to = self.chip * 2 + other
        self.go(send(mine, mine, self.s3.at[0], self.v3.at[0], to, self.rep))
        self.last = send(theirs, theirs, self.s3.at[0], self.v3.at[0], to, self.rep)

    def finish(self, out, direct=False):
        for copy in self.thirds if direct else [self.last]:
            copy.wait_recv()
        out[...] = self.got[...].reshape(self.n * self.ch, LANES)

    def drain(self):
        for copy in self.sends:
            copy.wait_send()
        self.sends = []


def put_grad(full, offset, grad, n_rep):
    share = grad.shape[0] // n_rep
    low = grad.astype(BF16)
    for j in range(grad.shape[1] // LANES):
        full[:, offset + j * share : offset + (j + 1) * share, :] = low[
            :, j * LANES : (j + 1) * LANES
        ].reshape(n_rep, share, LANES)


def half_rows(shape, n_rep):
    return shape[0] // n_rep * (shape[1] // 2 // LANES)


def take_grad(flat, offset, out, scale):
    share = out.shape[0]
    panels = out.shape[1] // 2 // LANES
    rows = flat.shape[0] // 2
    for c in range(2):
        for j in range(panels):
            at = c * rows + offset + j * share
            col = (c * panels + j) * LANES
            out[:, col : col + LANES] = flat[at : at + share].astype(F32) * scale


def kernel(
    n_graph, n_rep,
    *refs
):
    ins, outs, held, rest = refs[:12], refs[12:18], refs[18:30], refs[30:]
    live, partner, nodes, src_ref, dst_ref, we1, be, we2, wn1, bn, cot, wn2 = held
    updated_out, dnodes_out, flat_a, flat_b, flat_c, bias_out = outs
    (outgoing, arrived_low, arrived_high, keygrad, backsend, back, inv,
     msg_f, moved_f, gh_f, act_f, go_f, gat_f, gm_f, gts_f,
     nodes_s, msg_s, moved_s, gh_s, act_s, go_s, gat_s, gm_s, gts_s,
     nodes_t, msg_t, gat_t,
     bias_f, bias_g, bias_m, bias_r,
     load_sem, x_send, x_recv, b_send, b_recv, sib_send, sib_recv,
     c_send, c_recv, d_send, d_recv) = rest[:42]
    group_refs = rest[42:]
    arrived = (arrived_low, arrived_high)
    me = lax.axis_index("graph")
    rep = lax.axis_index("rep")
    core = lax.rem(me, 2)
    other = 1 - core
    sibling = me + other - core
    G, B, H = nodes.shape
    R = G * B
    half = G // 2
    E = src_ref.shape[1]
    FM = wn1.shape[1]
    per = len(group_refs) // 3
    ga = Group(n_graph, n_rep, me, rep, True, group_refs[:per])
    gb = Group(n_graph, n_rep, me, rep, True, group_refs[per : 2 * per])
    gc = Group(n_graph, n_rep, me, rep, False, group_refs[2 * per :])

    loads = []
    for i, (a, b) in enumerate(zip(ins, held)):
        copy = pltpu.make_async_copy(a, b, load_sem.at[i])
        copy.start()
        loads.append(copy)
    barrier = pltpu.get_barrier_semaphore()
    for d in range(1, n_graph):
        pl.semaphore_signal(barrier, inc=1, device_id={"graph": lax.rem(me + d, n_graph), "rep": rep},
                            device_id_type=pl.DeviceIdType.MESH)
    for d in range(1, n_rep):
        pl.semaphore_signal(barrier, inc=1, device_id={"graph": me, "rep": lax.rem(rep + d, n_rep)},
                            device_id_type=pl.DeviceIdType.MESH)
    for copy in loads[:3]:
        copy.wait()
    owner = [lax.div(partner[0, g], G) for g in range(G)]
    mark_row = lax.broadcasted_iota(jnp.int32, (B, LANES), 0)
    mark_lane = lax.broadcasted_iota(jnp.int32, (B, LANES), 1)

    def marked(g, count):
        mark = jnp.where(mark_row >= count, jnp.where(mark_lane == 0, MARK, 0.0), 0.0)
        return (nodes[g, :, :LANES].astype(F32) + mark).astype(BF16)

    def build(p, h):
        first = jnp.int32(0)
        count = jnp.int32(0)
        for g in reversed(range(h * half, (h + 1) * half)):
            hit = owner[g] == p
            first = jnp.where(hit, g, first)
            count = count + jnp.where(hit, 1, 0)
        inv[0, p * 2 + h] = first
        inv[1, p * 2 + h] = count
        second = jnp.minimum(first + 1, G - 1)
        outgoing[p, h, :B, :LANES] = marked(first, live[0, first])
        outgoing[p, h, B:, :LANES] = marked(second, jnp.where(count > 1, live[0, second], 0))
        outgoing[p, h, :B, LANES:] = nodes[first, :, LANES:]
        outgoing[p, h, B:, LANES:] = nodes[second, :, LANES:]

    pl.semaphore_wait(barrier, n_graph + n_rep - 2)

    sends = []
    key_waits = []
    for h in range(2):

        def ship(i, carry):
            d = lax.rem(i, n_graph - 1) + 1
            to = lax.rem(me + d, n_graph)
            build(to, h)
            send(outgoing.at[to, h], arrived[h].at[me], x_send.at[h * n_graph + d],
                 x_recv.at[h * n_graph + d], to, rep).start()
            return carry

        lax.fori_loop(1, n_graph, ship, 0)
        waits = []
        for d in range(1, n_graph):
            to = lax.rem(me + d, n_graph)
            frm = lax.rem(me + n_graph - d, n_graph)
            s_sem, r_sem = x_send.at[h * n_graph + d], x_recv.at[h * n_graph + d]
            sends.append(send(outgoing.at[to, h], arrived[h].at[me], s_sem, r_sem, to, rep))
            waits.append(send(outgoing.at[to, h], arrived[h].at[frm], s_sem, r_sem, to, rep))
        key_waits.append(waits)
        build(me, h)
        arrived[h][me] = outgoing[me, h]

    def share(i, src, dst):
        copy = send(src, dst, sib_send.at[i], sib_recv.at[i], sibling, rep)
        copy.start()
        sends.append(copy)
        return copy

    share_nodes = share(0, nodes, nodes_s)

    rows = nodes[...].reshape(R, H)
    loads[3].wait()
    loads[4].wait()
    row_ids = lax.broadcasted_iota(jnp.int32, (R, E), 0)
    hot = jnp.concatenate(
        [
            jnp.where(row_ids == dst_ref[...], 1.0, 0.0).astype(BF16),
            jnp.where(row_ids == src_ref[...], 1.0, 0.0).astype(BF16),
        ],
        axis=0,
    )
    hot_t = hot.T
    loads[5].wait()
    loads[6].wait()
    pre = jnp.concatenate(
        [
            (dot_nn(rows, we1[:H]) + be[...]).astype(BF16),
            dot_nn(rows, we1[H:]).astype(BF16),
        ],
        axis=0,
    )
    summed = dot_nn(hot_t, pre)
    edge_sig = sigmoid(summed)
    gathered = dot_nn(hot[:R], (summed * edge_sig).astype(BF16)).astype(BF16)
    gat_f[...] = gathered
    share_gat = share(1, gat_f, gat_s)
    loads[7].wait()
    message = dot_nn(gathered, we2[...]).astype(BF16)
    msg_f[...] = message
    share_msg = share(2, msg_f, msg_s)
    loads[8].wait()
    loads[9].wait()
    hidden_part = dot_nn(rows, wn1[:H]) + dot_nn(message, wn1[H : 2 * H]) + bn[...]
    position = lax.broadcasted_iota(jnp.int32, (B, H), 0)
    mask = jnp.concatenate(
        [jnp.where(position < live[0, g], 1.0, 0.0) for g in range(G)], axis=0
    ) > 0.5
    loads[10].wait()
    loads[11].wait()
    grad_out = jnp.where(mask, cot[...].reshape(R, H).astype(F32), 0.0).astype(BF16)
    for c in range(2):
        go_f[c] = grad_out[:, c * (H // 2) : (c + 1) * (H // 2)]
    share_go = share(3, go_f.at[other], go_s)
    back_hidden = dot_nt(grad_out, wn2[...])

    def two_cores(mine, theirs):
        return jnp.concatenate([mine, theirs], axis=0)

    for copy in (share_nodes, share_gat, share_msg, share_go):
        copy.wait_recv()
    nodes_t[...] = two_cores(rows, nodes_s[...].reshape(R, H)).T
    msg_t[...] = two_cores(message, msg_s[...]).T
    gat_t[...] = two_cores(gathered, gat_s[...]).T

    scale = H ** (-0.5)
    first_lane = lax.broadcasted_iota(jnp.int32, (16, H), 1) == 0
    pick = jnp.where(first_lane, 1.0, 0.0).astype(BF16)

    def keys_of(g):
        return arrived[1 if g < half else 0][owner[g]]

    def block(values, g):
        return values[g * B : (g + 1) * B]

    def attend(p):
        part = range(p * half, (p + 1) * half)
        at, to = p * half * B, (p + 1) * half * B
        products = [dot_nt(jnp.concatenate([block(rows, g), pick], axis=0), keys_of(g)) for g in part]
        marks = jnp.concatenate([jnp.broadcast_to(v[B : B + 1], (B, GMAX * B)) for v in products], axis=0)
        scores = jnp.concatenate([v[:B] for v in products], axis=0) * scale
        scores = jnp.where(marks < 0.5 * MARK, scores, -jnp.inf)
        powers = jnp.exp(scores - jnp.max(scores, axis=-1, keepdims=True))
        probs = powers / jnp.sum(powers, axis=-1, keepdims=True)
        low = probs.astype(BF16)
        context = jnp.concatenate(
            [dot_nn(low[i * B : (i + 1) * B], keys_of(g)) for i, g in enumerate(part)], axis=0
        )
        moved = (rows[at:to].astype(F32) - context).astype(BF16)
        moved_f[at:to, :] = moved
        hidden_pre = hidden_part[at:to] + dot_nn(moved, wn1[2 * H :])
        sig = sigmoid(hidden_pre)
        grad_hidden = (back_hidden[at:to] * silu_slope(hidden_pre, sig)).astype(BF16)
        for c in range(2):
            gh_f[c, at:to, :] = grad_hidden[:, c * (FM // 2) : (c + 1) * (FM // 2)]
        return probs, low, moved, grad_hidden, hidden_pre, sig

    def activate(p, hidden_pre, sig):
        active = (hidden_pre * sig).astype(BF16)
        act_f[p * half * B : (p + 1) * half * B, :] = active
        return active

    def message_back(p, grad_hidden):
        at, to = p * half * B, (p + 1) * half * B
        grad_message = dot_nt(grad_hidden, wn1[H : 2 * H]).astype(BF16)
        for c in range(2):
            gm_f[c, at:to, :] = grad_message[:, c * (H // 2) : (c + 1) * (H // 2)]
        return dot_nt(grad_message, we2[...]).astype(BF16)

    for copy in key_waits[0]:
        copy.wait_recv()
    def share_part(i, p, src, dst):
        part = pl.ds(p * half * B, half * B)
        return share(i, src.at[part], dst.at[part])

    def share_moves(p):
        return [share_part(9 + p, p, moved_f, moved_s), share_part(11 + p, p, gh_f.at[other], gh_s)]

    upper = attend(1)
    share_mine = share_moves(1)
    upper_active = activate(1, *upper[4:])
    share_act = [share_part(14, 1, act_f, act_s)]
    upper_gathered = message_back(1, upper[3])
    for copy in key_waits[1]:
        copy.wait_recv()
    lower = attend(0)
    share_mine += share_moves(0)
    lower_active = activate(0, *lower[4:])
    share_act += [share_part(13, 0, act_f, act_s)]
    lower_gathered = message_back(0, lower[3])
    share_gm = share(7, gm_f.at[other], gm_s)
    probs, low, moved, grad_hidden = (
        jnp.concatenate([a, b], axis=0) for a, b in zip(lower[:4], upper[:4])
    )
    active = jnp.concatenate([lower_active, upper_active], axis=0)

    def node_pieces(part, moved_rows, gh):
        return jnp.concatenate(
            [dot_nn(nodes_t[:, part], gh), dot_nn(msg_t[:, part], gh), dot_tn(moved_rows, gh)], axis=0
        )

    mine = node_pieces(slice(0, R), moved, gh_f[core])
    piece = dot_tn(active, go_f[core])
    grad_gathered = jnp.concatenate([lower_gathered, upper_gathered], axis=0)
    edge_grad = (dot_nn(hot_t[:, :R], grad_gathered) * silu_slope(summed, edge_sig)).astype(BF16)
    both = dot_nn(hot, edge_grad).astype(BF16)
    for c in range(2):
        gts_f[c] = both[:, c * (FM // 2) : (c + 1) * (FM // 2)]
    share_gts = share(8, gts_f.at[other], gts_s)
    grad_target, grad_source = both[:R], both[R:]

    for copy in share_mine:
        copy.wait_recv()
    put_grad(ga.full, 0, mine + node_pieces(slice(R, 2 * R), moved_s[...], gh_s[...]), n_rep)
    ga.first_plane()

    for copy in share_act:
        copy.wait_recv()
    piece = piece + dot_tn(act_s[...], go_s[...])
    put_grad(gc.full, 0, piece, n_rep)
    cut = piece.shape[0] // n_rep * (piece.shape[1] // LANES)
    gc.first_rep(0, 0, cut)

    share_gm.wait_recv()
    piece = dot_nn(gat_t[...], two_cores(gm_f[core], gm_s[...]))
    put_grad(gc.full, cut, piece, n_rep)
    gc.first_rep(1, cut, gc.full.shape[1])

    width = FM // n_rep
    sums = (jnp.sum(grad_hidden.astype(F32), axis=0, keepdims=True),
            jnp.sum(grad_target.astype(F32), axis=0, keepdims=True))
    for i in range(2):
        for z in range(n_rep):
            row = sums[i][:, z * width : (z + 1) * width]
            if width < LANES:
                row = jnp.concatenate([row, jnp.zeros((1, LANES - width), F32)], axis=1)
            bias_f[z, i : i + 1, :] = row
    bias_r[rep] = bias_f[rep]
    bias_waits = []
    for d in range(1, n_rep):
        to = lax.rem(rep + d, n_rep)
        frm = lax.rem(rep + n_rep - d, n_rep)
        copy = send(bias_f.at[to], bias_r.at[rep], d_send.at[d], d_recv.at[d], me, to)
        copy.start()
        sends.append(copy)
        bias_waits.append(send(bias_f.at[to], bias_r.at[frm], d_send.at[d], d_recv.at[d], me, to))

    share_gts.wait_recv()
    mine, theirs = gts_f[core], gts_s[...]
    pieces = jnp.concatenate(
        [dot_nn(nodes_t[...], two_cores(mine[:R], theirs[:R])),
         dot_nn(nodes_t[...], two_cores(mine[R:], theirs[R:]))],
        axis=0,
    )
    put_grad(gb.full, 0, pieces, n_rep)
    gb.first_plane()

    grad_moved = dot_nt(grad_hidden, wn1[2 * H :]).astype(BF16)
    negated = -grad_moved
    grad_probs = jnp.concatenate(
        [dot_nt(block(negated, g), keys_of(g)) for g in range(G)], axis=0
    )
    inner = jnp.sum(probs * grad_probs, axis=-1, keepdims=True)
    grad_scores = (probs * (grad_probs - inner) * scale).astype(BF16)
    for g in range(G):
        left = jnp.concatenate([block(low, g), block(grad_scores, g)], axis=0)
        right = jnp.concatenate([block(negated, g), block(rows, g)], axis=0)
        keygrad[g] = dot_tn(left, right)

    def ship_back(d, carry):
        to = lax.rem(me + d, n_graph)
        for h in range(2):
            first = inv[0, to * 2 + h]
            count = inv[1, to * 2 + h]
            one = jnp.where(count > 0, 1.0, 0.0)
            two = jnp.where(count > 1, 1.0, 0.0)
            total = keygrad[first] * one + keygrad[jnp.minimum(first + 1, G - 1)] * two
            backsend[to, (1 - h) * GMAX : (2 - h) * GMAX] = total.astype(BF16).reshape(GMAX, B, H)
        return carry

    lax.fori_loop(0, n_graph, ship_back, 0)
    back[me] = backsend[me]

    def start_back(h):
        waits = []
        for d in range(1, n_graph):
            to = lax.rem(me + d, n_graph)
            frm = lax.rem(me + n_graph - d, n_graph)
            part = pl.ds(h * GMAX, GMAX)
            s_sem, r_sem = b_send.at[h * n_graph + d], b_recv.at[h * n_graph + d]
            copy = send(backsend.at[to, part], back.at[me, part], s_sem, r_sem, to, rep)
            copy.start()
            sends.append(copy)
            waits.append(send(backsend.at[to, part], back.at[frm, part], s_sem, r_sem, to, rep))
        return waits

    back_waits = start_back(0)
    updated = jnp.where(mask, rows.astype(F32) + dot_nn(active, wn2[...]), 0.0)
    updated_out[...] = updated.astype(BF16).reshape(G, B, H)
    total = grad_out.astype(F32) + grad_moved.astype(F32)
    total = total + dot_nt(grad_hidden, wn1[:H])
    total = total + dot_nt(grad_target, we1[:H]) + dot_nt(grad_source, we1[H:])
    total = total + jnp.concatenate(
        [dot_nn(block(grad_scores, g), keys_of(g)) for g in range(G)], axis=0
    )

    ga.second()
    for copy in bias_waits:
        copy.wait_recv()
    summed_bias = bias_r[0]
    for z in range(1, n_rep):
        summed_bias = summed_bias + bias_r[z]
    bias_m[...] = summed_bias
    bias_g[me] = summed_bias
    bias_waits = []
    for d in range(1, n_graph):
        to = lax.rem(me + d, n_graph)
        frm = lax.rem(me + n_graph - d, n_graph)
        copy = send(bias_m, bias_g.at[me], c_send.at[d], c_recv.at[d], to, rep)
        copy.start()
        sends.append(copy)
        bias_waits.append(send(bias_m, bias_g.at[frm], c_send.at[d], c_recv.at[d], to, rep))
    gc.second()
    back_waits += start_back(1)
    gb.second()
    ga.drain()
    ga.gather()
    gc.drain()
    gc.gather()
    gb.drain()
    gb.gather(direct=True)
    ga.swap()
    gc.swap()
    for copy in back_waits:
        copy.wait_recv()
    returned = []
    for g in range(G):
        h = 0 if g < half else 1
        same = partner[0, g] == partner[0, g - 1] if g > 0 else False
        place = jnp.where(same, 1, 0)
        returned.append(back[owner[g], h * GMAX + place])
    total = total + jnp.concatenate(returned, axis=0).astype(F32)
    dnodes_out[...] = jnp.where(mask, total, 0.0).astype(BF16).reshape(G, B, H)
    for copy in bias_waits:
        copy.wait_recv()
    summed_bias = bias_g[0]
    for i in range(1, n_graph):
        summed_bias = summed_bias + bias_g[i]
    bias_out[...] = summed_bias
    for copy in sends:
        copy.wait_send()
    ga.finish(flat_a)
    gc.finish(flat_c)
    gb.finish(flat_b, direct=True)
    for group in (ga, gb, gc):
        group.drain()


def unpack(
    grad_scale, updated, dnodes, flat_a, flat_b, flat_c, bias,
    updated_out, dnodes_out, oe1, obe, oe2, on1, obn, on2,
    ve1, vbe, ve2, vn1, vbn, vn2, sem,
):
    copies = []

    def put(src, dst):
        copy = pltpu.make_async_copy(src, dst, sem.at[len(copies)])
        copy.start()
        copies.append(copy)

    put(updated, updated_out)
    put(dnodes, dnodes_out)
    take_grad(flat_a, 0, vn1, grad_scale)
    put(vn1, on1)
    take_grad(flat_b, 0, ve1, grad_scale)
    put(ve1, oe1)
    take_grad(flat_c, 0, vn2, grad_scale)
    put(vn2, on2)
    take_grad(flat_c, on2.shape[0] * (on2.shape[1] // 2 // LANES), ve2, grad_scale)
    put(ve2, oe2)
    vbn[...] = bias[0:1, : vbn.shape[1]] * grad_scale
    put(vbn, obn)
    vbe[...] = bias[1:2, : vbe.shape[1]] * grad_scale
    put(vbe, obe)
    for copy in copies:
        copy.wait()


def group_scratch(shapes, n_graph, n_rep, plane_first):
    chips = n_graph // 2
    rows = round_up(sum(half_rows(s, n_rep) for s in shapes), 16 * chips)
    ch = rows // chips
    dma = pltpu.SemaphoreType.DMA
    plane = (chips, n_rep, ch, LANES)
    if plane_first:
        middle = [plane, (n_rep, ch, LANES), (n_rep, ch, LANES)]
        first, second = chips, n_rep
    else:
        middle = [(n_rep, rows, LANES), (rows, LANES), (chips, ch, LANES)]
        first, second = len(shapes) * n_rep, chips
    return [pltpu.VMEM((n_rep, rows, LANES), BF16)] + [pltpu.VMEM(s, BF16) for s in middle] + [
        pltpu.VMEM((n_graph, ch, LANES), BF16),
        dma((first,)), dma((first,)), dma((second,)), dma((second,)), dma((n_graph,)), dma((n_graph,)),
    ]


def on_device(
    n_graph, n_rep,
    nodes, cotangent, live, partner_first, partner_size, edge_src, edge_dst,
    w_edge1, b_edge, w_edge2, w_node1, b_node, w_node2,
):
    _, G, B, H = nodes.shape
    FM = w_edge1.shape[1]
    R = G * B
    dma = pltpu.SemaphoreType.DMA
    vmem = pl.BlockSpec(memory_space=pltpu.VMEM)
    hbm = pl.BlockSpec(memory_space=pltpu.HBM)
    sds = jax.ShapeDtypeStruct

    def share(shape):
        return sds((shape[0] // n_rep,) + tuple(shape[1:]), F32)

    groups = [
        group_scratch([w_node1.shape], n_graph, n_rep, True),
        group_scratch([w_edge1.shape], n_graph, n_rep, True),
        group_scratch([w_node2.shape, w_edge2.shape], n_graph, n_rep, False),
    ]
    flats = tuple(sds((2 * g[0].shape[1], LANES), BF16) for g in groups)
    ints = [live, partner_first]
    arrays = [nodes[0], edge_src, edge_dst, w_edge1, b_edge.reshape(1, FM), w_edge2, w_node1,
              b_node.reshape(1, FM), cotangent[0], w_node2]

    def wide(*shape):
        return pltpu.VMEM(shape, F32)

    def bf(*shape):
        return pltpu.VMEM(shape, BF16)

    scratch = (
        [pltpu.SMEM(w.shape, w.dtype) for w in ints]
        + [pltpu.VMEM(w.shape, w.dtype) for w in arrays]
        + [
            bf(n_graph, 2, GMAX * B, H),
            bf(n_graph, GMAX * B, H),
            bf(n_graph, GMAX * B, H),
            wide(G, GMAX * B, H),
            bf(n_graph, 2 * GMAX, B, H),
            bf(n_graph, 2 * GMAX, B, H),
            pltpu.SMEM((2, 2 * n_graph), jnp.int32),
            bf(R, H), bf(R, H), bf(2, R, FM // 2), bf(R, FM), bf(2, R, H // 2), bf(R, FM),
            bf(2, R, H // 2), bf(2, 2 * R, FM // 2),
            bf(G, B, H), bf(R, H), bf(R, H), bf(R, FM // 2), bf(R, FM), bf(R, H // 2), bf(R, FM),
            bf(R, H // 2), bf(2 * R, FM // 2),
            bf(H, 2 * R), bf(H, 2 * R), bf(FM, 2 * R),
            wide(n_rep, 2, LANES), wide(n_graph, 2, LANES), wide(2, LANES), wide(n_rep, 2, LANES),
            dma((12,)),
            dma((2 * n_graph,)), dma((2 * n_graph,)),
            dma((2 * n_graph,)), dma((2 * n_graph,)), dma((15,)), dma((15,)),
            dma((n_graph,)), dma((n_graph,)), dma((n_rep,)), dma((n_rep,)),
        ]
        + sum(groups, [])
    )
    held = sum(math.prod(w.shape) * w.dtype.itemsize for w in scratch if w.dtype in (BF16, F32))
    parts = pl.pallas_call(
        functools.partial(kernel, n_graph, n_rep),
        out_shape=(sds((G, B, H), BF16), sds((G, B, H), BF16)) + flats + (sds((2, LANES), F32),),
        in_specs=[hbm] * 12,
        out_specs=(vmem,) * 6,
        scratch_shapes=scratch,
        compiler_params=pltpu.CompilerParams(
            collective_id=0, has_side_effects=True, vmem_limit_bytes=min(2 * held, 64 * 1000 * 1000)
        ),
    )(*[pltpu.with_memory_space_constraint(a, pltpu.HBM) for a in ints + arrays])
    shapes = (
        share(w_edge1.shape),
        sds((1, FM // n_rep), F32),
        share(w_edge2.shape),
        share(w_node1.shape),
        sds((1, FM // n_rep), F32),
        share(w_node2.shape),
    )
    outs = pl.pallas_call(
        functools.partial(unpack, (n_graph * n_rep * G * B) ** (-0.5)),
        out_shape=(sds((G, B, H), BF16), sds((G, B, H), BF16)) + shapes,
        in_specs=[vmem] * 6,
        out_specs=(hbm,) * 8,
        scratch_shapes=[pltpu.VMEM(w.shape, F32) for w in shapes] + [dma((8,))],
        compiler_params=pltpu.CompilerParams(vmem_limit_bytes=16 * 1000 * 1000),
    )(*parts)
    return (
        outs[0][None],
        outs[1][None],
        outs[2],
        outs[3].reshape(-1),
        outs[4],
        outs[5],
        outs[6].reshape(-1),
        outs[7],
    )


def solution(mesh):
    rows = P("rep", "graph", None, None)
    ints = P("rep", "graph")
    return jax.shard_map(
        functools.partial(on_device, mesh.shape["graph"], mesh.shape["rep"]),
        mesh=mesh,
        in_specs=(rows, rows, ints, ints, ints, ints, ints) + (P(),) * 6,
        out_specs=(
            rows,
            rows,
            P("rep", None),
            P("rep"),
            P("rep", None),
            P("rep", None),
            P("rep"),
            P("rep", None),
        ),
        check_vma=False,
    )
```
